256 devices in a mesh: mem: 64 (over x, z, core), chan: 4 (over y).
Axes of the slice: x: 4, y: 4, z: 8, core: 2. Of those that a mesh axis runs over, the one named last changes fastest.
Arguments:
- state_anom: bfloat16 [64, 512, 137], P(None, 'mem'), may hold values from -6 to 6
- radiance_anom: bfloat16 [64, 512, 8704], P(None, 'mem', 'chan'), may hold values from -6 to 6
- inv_noise: float32 [8704], P('chan'), may hold values from 0.02 to 0.2
- innovation: float32 [64, 8704], P(None, 'chan'), may hold values from -6 to 6
- valid_count: int32 [64], replicated, may hold values from 4352 to 8461
Outputs:
- information: float32 [64, 137, 137], P('mem')
- gradient: float32 [64, 137], P('mem')
- increment: float32 [64, 137], P('mem')
The draws below stay inside these ranges and needn't reach their ends.
All inputs are finite; a program needn't handle non-finite values.
Results may differ from the reference program's by a relative error of at most 0.0003.
Values may be sent and summed in bfloat16 or wider, within the bound.
No kernel may reach another device: no remote copies, remote signals or barrier semaphores. Data moves between devices by JAX's collectives and lax.ppermute only.
A program may use at most 64 MiB of HBM per device.

```python
import math
import jax
import jax.numpy as jnp
from jax import lax

STATE = 137
PROF = 64
MEMBERS = 512
CHANNELS = 8704


def place_ends(result, own_key, low, top_value):
    place = [jax.random.randint(jax.random.fold_in(own_key, axis), (), 0, length) for axis, length in enumerate(result.shape)]
    longest = result.shape.index(max(result.shape))
    neighbour = place[:longest] + [(place[longest] + 1) % result.shape[longest]] + place[longest + 1:]
    return result.at[tuple(place)].set(low).at[tuple(neighbour)].set(top_value)


def levels(stream_key, dims, pieces, least, top_value):
    loudness, own = 1.0, jax.random.fold_in(stream_key, 6)
    for position, shards_of in pieces:
        heights = jnp.exp(jax.random.uniform(jax.random.fold_in(own, position), (shards_of,), jnp.float32, least / len(pieces), top_value / len(pieces)))
        loudness = loudness * jnp.repeat(heights, dims[position] // shards_of).reshape([-1 if axis == position else 1 for axis in range(len(dims))])
    return loudness


def bell_draw(rng, dims, deviation, reach, pieces=(), held_as=jnp.bfloat16):
    array = jax.random.normal(rng, dims, jnp.float32) * deviation
    if len(pieces) > 0:
        array = levels(rng, dims, pieces, -0.22, 0.18) * array
    return jnp.clip(array, min=-reach, max=reach).astype(held_as)


def setup_inputs(seed: int = 0) -> dict:
    keys = jax.random.split(jax.random.key(seed), 6)
    return {
        "state_anom": bell_draw(keys[0], (PROF, MEMBERS, STATE), 1.0, 6.0, ((1, 64),)),
        "radiance_anom": bell_draw(keys[1], (PROF, MEMBERS, CHANNELS), 1.0, 6.0, ((1, 64), (2, 4))),
        "inv_noise": jnp.clip(jnp.exp(math.log(0.2) - 2.3025851 * jax.random.uniform(keys[2], (CHANNELS,), jnp.float32) ** levels(keys[2], (CHANNELS,), ((0, 4),), -0.2, 0.2)), 0.02, 0.2),
        "innovation": bell_draw(keys[3], (PROF, CHANNELS), 1.0, 6.0, ((1, 4),), jnp.float32),
        "valid_count": place_ends(jax.random.randint(keys[4], (PROF,), CHANNELS // 2, min(CHANNELS, 8461) + 1), jax.random.fold_in(keys[4], 1), CHANNELS // 2, min(CHANNELS, 8461)).astype(jnp.int32),
    }


def reference(state_anom, radiance_anom, inv_noise, innovation, valid_count):
    cross = jnp.einsum('pmc,pms->pcs', radiance_anom.astype(jnp.float32), state_anom.astype(jnp.float32), precision=lax.Precision.HIGHEST)
    cross = cross / jnp.float32(MEMBERS - 1)
    slots = jnp.arange(CHANNELS, dtype=jnp.int32)
    valid = (slots[None, :] < valid_count[:, None].astype(jnp.int32)).astype(jnp.float32)
    weight = inv_noise[None, :] * valid
    weighted = cross * weight[:, :, None]
    information = jnp.einsum('pcs,pct->pst', weighted, cross, precision=lax.Precision.HIGHEST)
    gradient = jnp.einsum('pcs,pc->ps', weighted, innovation, precision=lax.Precision.HIGHEST)
    system = information + jnp.eye(STATE, dtype=jnp.float32)[None]
    increment = jnp.linalg.solve(system, gradient[:, :, None])[:, :, 0]
    return (information, gradient, increment)
```

```python
import functools

import jax
import jax.numpy as jnp
from jax import lax
from jax.experimental import pallas as pl
from jax.experimental.pallas import tpu as pltpu
from jax.sharding import PartitionSpec as P

LANES = 128
TOL = 1e-5
FIRST_STEPS = 10
MORE_STEPS = 4
MORE_ROUNDS = 8


def diagonal(rows):
    r = lax.broadcasted_iota(jnp.int32, (rows, LANES), 0)
    c = lax.broadcasted_iota(jnp.int32, (rows, LANES), 1)
    return r, c


def slab_kernel(states, members_all, x_ref, weight_ref, innov_ref, out_ref):
    width = weight_ref.shape[1]
    rad = x_ref[:, 0:width]
    st = x_ref[:, width : width + states]
    cross = lax.dot_general(st, rad, (((0,), (0,)), ((), ())), preferred_element_type=jnp.float32)
    root = jnp.sqrt(weight_ref[...])
    y = cross * (root * (1.0 / (members_all - 1)))
    y1 = y.astype(jnp.bfloat16)
    y2 = (y - y1.astype(jnp.float32)).astype(jnp.bfloat16)
    nt = (((1,), (1,)), ((), ()))
    main = lax.dot_general(y1, y1, nt, preferred_element_type=jnp.float32)
    side = lax.dot_general(y2, y1, nt, preferred_element_type=jnp.float32)
    info = main + (side + side.T)
    grad = jnp.sum(y * (root * innov_ref[...]), axis=1, keepdims=True)
    r = lax.broadcasted_iota(jnp.int32, info.shape, 0)
    c = lax.broadcasted_iota(jnp.int32, info.shape, 1)
    grad_row = jnp.sum(jnp.where(r == c, grad, 0.0), axis=0, keepdims=True)
    rest = states - LANES
    out_ref[...] = jnp.zeros_like(out_ref)
    out_ref[0:states, :] = info[:, 0:LANES]
    out_ref[states : states + 1, :] = grad_row[:, 0:LANES]
    out_ref[LANES + 16 : LANES + 16 + rest, 0:rest] = info[LANES:states, LANES:states]
    out_ref[LANES + 16 + rest : LANES + 17 + rest, 0:rest] = grad_row[:, LANES:states]


def solve_kernel(states, a_ref, b_ref, c_ref, d_ref, info_ref, grad_ref, inc_ref, left, right, x_ref, r_ref, p_ref, gj):
    rest = states - LANES
    rows = LANES + 16
    total = (a_ref[...] + c_ref[...]) + (b_ref[...] + d_ref[...])
    r, c = diagonal(16)
    low = jnp.where(r < rest, total[LANES:rows, :], 0.0)
    corner = jnp.where((r < rest) & (c < rest), total[rows : rows + 16, :], 0.0)
    g0 = total[states : states + 1, :]
    g1 = total[rows + rest : rows + rest + 1, :]
    upper = jnp.concatenate([low, jnp.zeros((LANES - 16, LANES), jnp.float32)], axis=0).T
    info_ref[:, 0, 0:LANES] = jnp.concatenate([total[0:LANES], low[0:rest]], axis=0)
    info_ref[:, 0, LANES:states] = jnp.concatenate([upper[:, 0:rest], corner[0:rest, 0:rest]], axis=0)
    grad_ref[:, 0:LANES] = g0
    grad_ref[:, LANES:states] = g1[:, 0:rest]
    ra, ca = diagonal(LANES)
    eye = (ra == ca).astype(jnp.float32)
    eye_low = (r == c).astype(jnp.float32)
    left[0:LANES, :] = total[0:LANES] + eye
    left[LANES:rows, :] = low
    right[0:LANES, :] = upper
    right[LANES:rows, :] = corner + eye_low

    def to_rows(v):
        return (
            jnp.sum(v[0:LANES] * eye, axis=0, keepdims=True),
            jnp.sum(v[LANES:rows] * eye_low, axis=0, keepdims=True),
        )

    def times(v):
        v0, v1 = to_rows(v)
        return jnp.broadcast_to(jnp.sum(left[...] * v0 + right[...] * v1, axis=1, keepdims=True), (rows, LANES))

    def dot(u, v):
        return jnp.sum(u * v, axis=0, keepdims=True)

    def ratio(num, den):
        return jnp.where(den > 0.0, num / jnp.where(den > 0.0, den, 1.0), 0.0)

    def steps(n, x, res, p, rr):
        for _ in range(n):
            q = times(p)
            alpha = ratio(rr, dot(p, q))
            x = x + alpha * p
            res = res - alpha * q
            new = dot(res, res)
            p = res + ratio(new, rr) * p
            rr = new
        return x, res, p, rr

    col = jnp.concatenate(
        [
            jnp.broadcast_to(jnp.sum(eye * g0, axis=1, keepdims=True), (LANES, LANES)),
            jnp.broadcast_to(jnp.sum(jnp.where(c < rest, eye_low * g1, 0.0), axis=1, keepdims=True), (16, LANES)),
        ],
        axis=0,
    )

    def put(x):
        x0, x1 = to_rows(x)
        inc_ref[:, 0:LANES] = x0
        inc_ref[:, LANES:states] = x1[:, 0:rest]

    def open_after(x):
        res = col - times(x)
        bad = jnp.logical_not(dot(res, res) <= (TOL * TOL) * dot(x, x))
        return jnp.max(bad[:, 0:1].astype(jnp.int32))

    x, res, p, rr = steps(FIRST_STEPS, jnp.zeros_like(col), col, col, dot(col, col))
    put(x)
    still = open_after(x)

    @pl.when(still > 0)
    def _():
        x_ref[...] = x
        r_ref[...] = res
        p_ref[...] = p

        def more(state):
            k, _ = state
            res = r_ref[...]
            x, res, p, _ = steps(MORE_STEPS, x_ref[...], res, p_ref[...], dot(res, res))
            x_ref[...] = x
            r_ref[...] = res
            p_ref[...] = p
            return k + 1, open_after(x)

        _, open_still = lax.while_loop(
            lambda s: (s[0] < MORE_ROUNDS) & (s[1] > 0), more, (jnp.int32(0), jnp.int32(1))
        )
        put(x_ref[...])

        @pl.when(open_still > 0)
        def _():
            wide_r = lax.broadcasted_iota(jnp.int32, (rows, 3 * LANES), 0)
            wide_c = lax.broadcasted_iota(jnp.int32, (rows, 3 * LANES), 1)
            gj[:, 0:LANES] = left[...]
            gj[:, LANES : 2 * LANES] = right[...]
            gj[:, 2 * LANES : 3 * LANES] = col

            def eliminate(i, _):
                a = gj[...]
                row = jnp.sum(jnp.where(wide_r == i, a, 0.0), axis=0, keepdims=True)
                lane = lax.broadcasted_iota(jnp.int32, row.shape, 1)
                pivot = jnp.sum(jnp.where(lane == i, row, 0.0), axis=1, keepdims=True)
                row = row / pivot
                column = jnp.sum(jnp.where(wide_c == i, a, 0.0), axis=1, keepdims=True)
                gj[...] = jnp.where(wide_r == i, row, a - column * row)
                return 0

            lax.fori_loop(0, states, eliminate, 0)
            put(gj[:, 2 * LANES : 3 * LANES])


def shards(state_anom, radiance_anom, inv_noise, innovation, valid_count):
    profiles, local_members, states = state_anom.shape
    slab_width = radiance_anom.shape[2]
    mem = lax.axis_size("mem")
    chan = lax.axis_size("chan")
    members_all = local_members * mem
    f32 = jnp.float32
    both = jnp.concatenate([radiance_anom, state_anom], axis=2)
    own = lax.all_to_all(both, "mem", split_axis=0, concat_axis=1, tiled=True)
    prof = lax.axis_index("mem")
    own_count = lax.dynamic_slice_in_dim(valid_count, prof, 1, 0)
    slots = lax.axis_index("chan") * slab_width + jnp.arange(slab_width, dtype=jnp.int32)
    weight = jnp.where(slots[None, :] < own_count[:, None], inv_noise[None, :], 0.0)
    innov = lax.dynamic_slice_in_dim(innovation, prof, 1, 0)
    rows = LANES + 32
    part = pl.pallas_call(
        functools.partial(slab_kernel, states, members_all),
        out_shape=jax.ShapeDtypeStruct((rows, LANES), f32),
        in_specs=[pl.BlockSpec(memory_space=pltpu.VMEM)] * 3,
        out_specs=pl.BlockSpec(memory_space=pltpu.VMEM),
        name="slab",
    )(own[0], weight, innov)
    parts = [part] + [
        lax.ppermute(part, "chan", [(j, (j + k) % chan) for j in range(chan)]) for k in range(1, chan)
    ]
    square = pltpu.VMEM((LANES + 16, LANES), f32)
    info, grad, inc = pl.pallas_call(
        functools.partial(solve_kernel, states),
        out_shape=[
            jax.ShapeDtypeStruct((states, 1, states), f32),
            jax.ShapeDtypeStruct((1, states), f32),
            jax.ShapeDtypeStruct((1, states), f32),
        ],
        in_specs=[pl.BlockSpec(memory_space=pltpu.VMEM)] * 4,
        out_specs=[pl.BlockSpec(memory_space=pltpu.VMEM)] * 3,
        scratch_shapes=[square] * 5 + [pltpu.VMEM((LANES + 16, 3 * LANES), f32)],
        name="solve",
    )(*parts)
    return (jnp.transpose(info, (1, 0, 2)), grad, inc)


def solution(mesh):
    in_specs = (P(None, "mem", None), P(None, "mem", "chan"), P("chan"), P(None, "chan"), P())
    out_specs = (P("mem", None, None), P("mem", None), P("mem", None))
    return jax.shard_map(shards, mesh=mesh, in_specs=in_specs, out_specs=out_specs, check_vma=False)
```

```python
import functools

import jax
import jax.numpy as jnp
from jax import lax
from jax.experimental import pallas as pl
from jax.experimental.pallas import tpu as pltpu
from jax.sharding import PartitionSpec as P

LANES = 128
TOL = 1e-5
FIRST_STEPS = 10
MORE_STEPS = 4
MORE_ROUNDS = 8


def diagonal(rows):
    r = lax.broadcasted_iota(jnp.int32, (rows, LANES), 0)
    c = lax.broadcasted_iota(jnp.int32, (rows, LANES), 1)
    return r, c


PIECES = 8


def join_kernel(rad_ref, st_ref, out_ref, held, st, arrived, left):
    width = rad_ref.shape[2]
    states = st_ref.shape[2]
    step = rad_ref.shape[0] // PIECES
    first = pltpu.make_async_copy(st_ref, st, arrived.at[PIECES])
    first.start()
    into, away = [], []
    for k in range(PIECES):
        part = pl.ds(k * step, step)
        into.append(pltpu.make_async_copy(rad_ref.at[part], held.at[part, :, pl.ds(0, width)], arrived.at[k]))
        away.append(pltpu.make_async_copy(held.at[part], out_ref.at[part], left.at[k]))
    for copy in into:
        copy.start()
    first.wait()
    held[:, :, width : width + states] = st[...]
    for come, go in zip(into, away):
        come.wait()
        go.start()
    for copy in away:
        copy.wait()


def slab_kernel(states, members_all, x_ref, weight_ref, innov_ref, out_ref):
    width = weight_ref.shape[1]
    rad = x_ref[:, 0:width]
    st = x_ref[:, width : width + states]
    cross = lax.dot_general(st, rad, (((0,), (0,)), ((), ())), preferred_element_type=jnp.float32)
    root = jnp.sqrt(weight_ref[...])
    y = cross * (root * (1.0 / (members_all - 1)))
    y1 = y.astype(jnp.bfloat16)
    y2 = (y - y1.astype(jnp.float32)).astype(jnp.bfloat16)
    nt = (((1,), (1,)), ((), ()))
    main = lax.dot_general(y1, y1, nt, preferred_element_type=jnp.float32)
    side = lax.dot_general(y2, y1, nt, preferred_element_type=jnp.float32)
    info = main + (side + side.T)
    grad = jnp.sum(y * (root * innov_ref[...]), axis=1, keepdims=True)
    r = lax.broadcasted_iota(jnp.int32, info.shape, 0)
    c = lax.broadcasted_iota(jnp.int32, info.shape, 1)
    grad_row = jnp.sum(jnp.where(r == c, grad, 0.0), axis=0, keepdims=True)
    rest = states - LANES
    out_ref[...] = jnp.zeros_like(out_ref)
    out_ref[0:states, :] = info[:, 0:LANES]
    out_ref[states : states + 1, :] = grad_row[:, 0:LANES]
    out_ref[LANES + 16 : LANES + 16 + rest, 0:rest] = info[LANES:states, LANES:states]
    out_ref[LANES + 16 + rest : LANES + 17 + rest, 0:rest] = grad_row[:, LANES:states]


def solve_kernel(states, a_ref, b_ref, c_ref, d_ref, info_ref, grad_ref, inc_ref, left, right, x_ref, r_ref, p_ref, gj):
    rest = states - LANES
    rows = LANES + 16
    total = (a_ref[...] + c_ref[...]) + (b_ref[...] + d_ref[...])
    r, c = diagonal(16)
    low = jnp.where(r < rest, total[LANES:rows, :], 0.0)
    corner = jnp.where((r < rest) & (c < rest), total[rows : rows + 16, :], 0.0)
    g0 = total[states : states + 1, :]
    g1 = total[rows + rest : rows + rest + 1, :]
    upper = jnp.concatenate([low, jnp.zeros((LANES - 16, LANES), jnp.float32)], axis=0).T
    info_ref[:, 0, 0:LANES] = jnp.concatenate([total[0:LANES], low[0:rest]], axis=0)
    info_ref[:, 0, LANES:states] = jnp.concatenate([upper[:, 0:rest], corner[0:rest, 0:rest]], axis=0)
    grad_ref[:, 0:LANES] = g0
    grad_ref[:, LANES:states] = g1[:, 0:rest]
    ra, ca = diagonal(LANES)
    eye = (ra == ca).astype(jnp.float32)
    eye_low = (r == c).astype(jnp.float32)
    left[0:LANES, :] = total[0:LANES] + eye
    left[LANES:rows, :] = low
    right[0:LANES, :] = upper
    right[LANES:rows, :] = corner + eye_low

    def to_rows(v):
        return (
            jnp.sum(v[0:LANES] * eye, axis=0, keepdims=True),
            jnp.sum(v[LANES:rows] * eye_low, axis=0, keepdims=True),
        )

    def times(v):
        v0, v1 = to_rows(v)
        return jnp.broadcast_to(jnp.sum(left[...] * v0 + right[...] * v1, axis=1, keepdims=True), (rows, LANES))

    def dot(u, v):
        return jnp.sum(u * v, axis=0, keepdims=True)

    def ratio(num, den):
        return jnp.where(den > 0.0, num / jnp.where(den > 0.0, den, 1.0), 0.0)

    def steps(n, x, res, p, rr):
        for _ in range(n):
            q = times(p)
            alpha = ratio(rr, dot(p, q))
            x = x + alpha * p
            res = res - alpha * q
            new = dot(res, res)
            p = res + ratio(new, rr) * p
            rr = new
        return x, res, p, rr

    col = jnp.concatenate(
        [
            jnp.broadcast_to(jnp.sum(eye * g0, axis=1, keepdims=True), (LANES, LANES)),
            jnp.broadcast_to(jnp.sum(jnp.where(c < rest, eye_low * g1, 0.0), axis=1, keepdims=True), (16, LANES)),
        ],
        axis=0,
    )

    def put(x):
        x0, x1 = to_rows(x)
        inc_ref[:, 0:LANES] = x0
        inc_ref[:, LANES:states] = x1[:, 0:rest]

    def open_after(x):
        res = col - times(x)
        bad = jnp.logical_not(dot(res, res) <= (TOL * TOL) * dot(x, x))
        return jnp.max(bad[:, 0:1].astype(jnp.int32))

    x, res, p, rr = steps(FIRST_STEPS, jnp.zeros_like(col), col, col, dot(col, col))
    put(x)
    still = open_after(x)

    @pl.when(still > 0)
    def _():
        x_ref[...] = x
        r_ref[...] = res
        p_ref[...] = p

        def more(state):
            k, _ = state
            res = r_ref[...]
            x, res, p, _ = steps(MORE_STEPS, x_ref[...], res, p_ref[...], dot(res, res))
            x_ref[...] = x
            r_ref[...] = res
            p_ref[...] = p
            return k + 1, open_after(x)

        _, open_still = lax.while_loop(
            lambda s: (s[0] < MORE_ROUNDS) & (s[1] > 0), more, (jnp.int32(0), jnp.int32(1))
        )
        put(x_ref[...])

        @pl.when(open_still > 0)
        def _():
            wide_r = lax.broadcasted_iota(jnp.int32, (rows, 3 * LANES), 0)
            wide_c = lax.broadcasted_iota(jnp.int32, (rows, 3 * LANES), 1)
            gj[:, 0:LANES] = left[...]
            gj[:, LANES : 2 * LANES] = right[...]
            gj[:, 2 * LANES : 3 * LANES] = col

            def eliminate(i, _):
                a = gj[...]
                row = jnp.sum(jnp.where(wide_r == i, a, 0.0), axis=0, keepdims=True)
                lane = lax.broadcasted_iota(jnp.int32, row.shape, 1)
                pivot = jnp.sum(jnp.where(lane == i, row, 0.0), axis=1, keepdims=True)
                row = row / pivot
                column = jnp.sum(jnp.where(wide_c == i, a, 0.0), axis=1, keepdims=True)
                gj[...] = jnp.where(wide_r == i, row, a - column * row)
                return 0

            lax.fori_loop(0, states, eliminate, 0)
            put(gj[:, 2 * LANES : 3 * LANES])


def shards(state_anom, radiance_anom, inv_noise, innovation, valid_count):
    profiles, local_members, states = state_anom.shape
    slab_width = radiance_anom.shape[2]
    mem = lax.axis_size("mem")
    chan = lax.axis_size("chan")
    members_all = local_members * mem
    f32 = jnp.float32
    both = pl.pallas_call(
        join_kernel,
        out_shape=jax.ShapeDtypeStruct((profiles, local_members, slab_width + 2 * LANES), jnp.bfloat16),
        in_specs=[pl.BlockSpec(memory_space=pltpu.HBM)] * 2,
        out_specs=pl.BlockSpec(memory_space=pltpu.HBM),
        scratch_shapes=[
            pltpu.VMEM((profiles, local_members, slab_width + 2 * LANES), jnp.bfloat16),
            pltpu.VMEM((profiles, local_members, states), jnp.bfloat16),
            pltpu.SemaphoreType.DMA((PIECES + 1,)),
            pltpu.SemaphoreType.DMA((PIECES,)),
        ],
        name="join",
    )(radiance_anom, state_anom)
    own = lax.all_to_all(both, "mem", split_axis=0, concat_axis=1, tiled=True)
    prof = lax.axis_index("mem")
    own_count = lax.dynamic_slice_in_dim(valid_count, prof, 1, 0)
    slots = lax.axis_index("chan") * slab_width + jnp.arange(slab_width, dtype=jnp.int32)
    weight = jnp.where(slots[None, :] < own_count[:, None], inv_noise[None, :], 0.0)
    innov = lax.dynamic_slice_in_dim(innovation, prof, 1, 0)
    rows = LANES + 32
    part = pl.pallas_call(
        functools.partial(slab_kernel, states, members_all),
        out_shape=jax.ShapeDtypeStruct((rows, LANES), f32),
        in_specs=[pl.BlockSpec(memory_space=pltpu.VMEM)] * 3,
        out_specs=pl.BlockSpec(memory_space=pltpu.VMEM),
        compiler_params=pltpu.CompilerParams(vmem_limit_bytes=24 * 2**20),
        name="slab",
    )(own[0], weight, innov)
    parts = [part] + [
        lax.ppermute(part, "chan", [(j, (j + k) % chan) for j in range(chan)]) for k in range(1, chan)
    ]
    square = pltpu.VMEM((LANES + 16, LANES), f32)
    info, grad, inc = pl.pallas_call(
        functools.partial(solve_kernel, states),
        out_shape=[
            jax.ShapeDtypeStruct((states, 1, states), f32),
            jax.ShapeDtypeStruct((1, states), f32),
            jax.ShapeDtypeStruct((1, states), f32),
        ],
        in_specs=[pl.BlockSpec(memory_space=pltpu.VMEM)] * 4,
        out_specs=[pl.BlockSpec(memory_space=pltpu.VMEM)] * 3,
        scratch_shapes=[square] * 5 + [pltpu.VMEM((LANES + 16, 3 * LANES), f32)],
        compiler_params=pltpu.CompilerParams(vmem_limit_bytes=8 * 2**20),
        name="solve",
    )(*parts)
    return (jnp.transpose(info, (1, 0, 2)), grad, inc)


def solution(mesh):
    in_specs = (P(None, "mem", None), P(None, "mem", "chan"), P("chan"), P(None, "chan"), P())
    out_specs = (P("mem", None, None), P("mem", None), P("mem", None))
    return jax.shard_map(shards, mesh=mesh, in_specs=in_specs, out_specs=out_specs, check_vma=False)
```

```python
import functools

import jax
import jax.numpy as jnp
from jax import lax
from jax.experimental import pallas as pl
from jax.experimental.pallas import tpu as pltpu
from jax.sharding import PartitionSpec as P

LANES = 128
TOL = 1e-5
FIRST_STEPS = 10
MORE_STEPS = 6
MORE_ROUNDS = 8
PACKED = 96


def places(rows):
    r = lax.broadcasted_iota(jnp.int32, (rows, LANES), 0)
    c = lax.broadcasted_iota(jnp.int32, (rows, LANES), 1)
    return r, c


PIECES = 8


def join_kernel(rad_ref, st_ref, out_ref, held, st, arrived, left):
    width = rad_ref.shape[2]
    states = st_ref.shape[2]
    step = rad_ref.shape[0] // PIECES
    first = pltpu.make_async_copy(st_ref, st, arrived.at[PIECES])
    first.start()
    into, away = [], []
    for k in range(PIECES):
        part = pl.ds(k * step, step)
        into.append(pltpu.make_async_copy(rad_ref.at[part], held.at[part, :, pl.ds(0, width)], arrived.at[k]))
        away.append(pltpu.make_async_copy(held.at[part], out_ref.at[part], left.at[k]))
    for copy in into:
        copy.start()
    first.wait()
    held[:, :, width : width + states] = st[...]
    for come, go in zip(into, away):
        come.wait()
        go.start()
    for copy in away:
        copy.wait()


def slab_kernel(states, members_all, x_ref, weight_ref, innov_ref, out_ref):
    width = weight_ref.shape[1]
    rad = x_ref[:, 0:width]
    st = x_ref[:, width : width + states]
    cross = lax.dot_general(st, rad, (((0,), (0,)), ((), ())), preferred_element_type=jnp.float32)
    root = jnp.sqrt(weight_ref[...])
    y = cross * (root * (1.0 / (members_all - 1)))
    y1 = y.astype(jnp.bfloat16)
    y2 = (y - y1.astype(jnp.float32)).astype(jnp.bfloat16)
    nt = (((1,), (1,)), ((), ()))
    main = lax.dot_general(y1, y1, nt, preferred_element_type=jnp.float32)
    side = lax.dot_general(y2, y1, nt, preferred_element_type=jnp.float32)
    info = main + (side + side.T)
    grad = jnp.sum(y * (root * innov_ref[...]), axis=1, keepdims=True)
    r = lax.broadcasted_iota(jnp.int32, info.shape, 0)
    c = lax.broadcasted_iota(jnp.int32, info.shape, 1)
    grad_row = jnp.sum(jnp.where(r == c, grad, 0.0), axis=0, keepdims=True)
    rest = states - LANES
    half = LANES // 2
    other = pltpu.roll(info[half:LANES, 0:LANES], half, 1)
    r, c = places(half)
    out_ref[0:half, :] = jnp.where(c < r, other, info[0:half, 0:LANES])
    out_ref[half:, :] = jnp.zeros((PACKED - half, LANES), jnp.float32)
    out_ref[half : half + rest, :] = info[LANES:states, 0:LANES]
    out_ref[half + rest : half + rest + 1, :] = grad_row[:, 0:LANES]
    out_ref[half + rest + 1 : half + rest + 2, :] = jnp.sum(jnp.where(r == c, other, 0.0), axis=0, keepdims=True)
    out_ref[half + 16 : half + 16 + rest, 0:rest] = info[LANES:states, LANES:states]
    out_ref[half + 16 + rest : half + 17 + rest, 0:rest] = grad_row[:, LANES:states]


def solve_kernel(
    states, a_ref, b_ref, c_ref, d_ref, info_ref, grad_ref, inc_ref, info, grad, inc, left, right, x_ref, r_ref, gj, done
):
    rest = states - LANES
    rows = LANES + 16
    half = LANES // 2
    total = (a_ref[...] + b_ref[...]) + (c_ref[...] + d_ref[...])
    r, c = places(half)
    ra, ca = places(LANES)
    last = jnp.where(ca[0:1] < half, total[half + rest + 1 : half + rest + 2, :], 0.0)
    lower = jnp.where(c < r, total[0:half], 0.0) + jnp.where(c == r, last, 0.0)
    part = jnp.concatenate([jnp.where(c < r, 0.0, total[0:half]), pltpu.roll(lower, half, 1)], axis=0)
    square = jnp.where(ra == ca, part, part + part.T)
    r, c = places(16)
    low = jnp.where(r < rest, total[half : half + 16, :], 0.0)
    corner = jnp.where((r < rest) & (c < rest), total[half + 16 : half + 32, :], 0.0)
    g0 = total[half + rest : half + rest + 1, :]
    g1 = total[half + 16 + rest : half + 17 + rest, :]
    upper = jnp.concatenate([low, jnp.zeros((LANES - 16, LANES), jnp.float32)], axis=0).T
    info[:, 0, 0:LANES] = jnp.concatenate([square, low[0:rest]], axis=0)
    info[:, 0, LANES:states] = jnp.concatenate([upper[:, 0:rest], corner[0:rest, 0:rest]], axis=0)
    grad[:, 0:LANES] = g0
    grad[:, LANES:states] = g1[:, 0:rest]
    eye = (ra == ca).astype(jnp.float32)
    eye_low = (r == c).astype(jnp.float32)
    left[0:LANES, :] = square + eye
    left[LANES:rows, :] = low
    right[0:LANES, :] = upper
    right[LANES:rows, :] = corner + eye_low
    early = (
        pltpu.make_async_copy(info, info_ref, done.at[0]),
        pltpu.make_async_copy(grad, grad_ref, done.at[1]),
    )
    for copy in early:
        copy.start()

    def to_rows(v):
        return (
            jnp.sum(v[0:LANES] * eye, axis=0, keepdims=True),
            jnp.sum(v[LANES:rows] * eye_low, axis=0, keepdims=True),
        )

    def times(v):
        v0, v1 = to_rows(v)
        return jnp.broadcast_to(jnp.sum(left[...] * v0 + right[...] * v1, axis=1, keepdims=True), (rows, LANES))

    def dot(u, v):
        return jnp.sum(u * v, axis=0, keepdims=True)

    def ratio(num, den):
        return jnp.where(den > 0.0, num / jnp.where(den > 0.0, den, 1.0), 0.0)

    def steps(n, x, res, p, s, gamma, alpha):
        for _ in range(n):
            w = times(res)
            new = dot(res, res)
            delta = dot(res, w)
            if gamma is None:
                alpha = ratio(new, delta)
                p, s = res, w
            else:
                beta = ratio(new, gamma)
                alpha = ratio(new, delta - beta * ratio(new, alpha))
                p = res + beta * p
                s = w + beta * s
            x = x + alpha * p
            res = res - alpha * s
            gamma = new
        return x, res

    col = jnp.concatenate(
        [
            jnp.broadcast_to(jnp.sum(eye * g0, axis=1, keepdims=True), (LANES, LANES)),
            jnp.broadcast_to(jnp.sum(jnp.where(c < rest, eye_low * g1, 0.0), axis=1, keepdims=True), (16, LANES)),
        ],
        axis=0,
    )

    def put(x):
        x0, x1 = to_rows(x)
        inc[:, 0:LANES] = x0
        inc[:, LANES:states] = x1[:, 0:rest]

    def open_after(x):
        res = col - times(x)
        bad = jnp.logical_not(dot(res, res) <= (TOL * TOL) * dot(x, x))
        return jnp.max(bad[:, 0:1].astype(jnp.int32)), res

    x, _ = steps(FIRST_STEPS, jnp.zeros_like(col), col, None, None, None, None)
    put(x)
    still, res = open_after(x)

    @pl.when(still > 0)
    def _():
        x_ref[...] = x
        r_ref[...] = res

        def more(state):
            k, _ = state
            x, _ = steps(MORE_STEPS, x_ref[...], r_ref[...], None, None, None, None)
            still, res = open_after(x)
            x_ref[...] = x
            r_ref[...] = res
            return k + 1, still

        _, open_still = lax.while_loop(
            lambda s: (s[0] < MORE_ROUNDS) & (s[1] > 0), more, (jnp.int32(0), jnp.int32(1))
        )
        put(x_ref[...])

        @pl.when(open_still > 0)
        def _():
            wide_r = lax.broadcasted_iota(jnp.int32, (rows, 3 * LANES), 0)
            wide_c = lax.broadcasted_iota(jnp.int32, (rows, 3 * LANES), 1)
            gj[:, 0:LANES] = left[...]
            gj[:, LANES : 2 * LANES] = right[...]
            gj[:, 2 * LANES : 3 * LANES] = col

            def eliminate(i, _):
                a = gj[...]
                row = jnp.sum(jnp.where(wide_r == i, a, 0.0), axis=0, keepdims=True)
                lane = lax.broadcasted_iota(jnp.int32, row.shape, 1)
                pivot = jnp.sum(jnp.where(lane == i, row, 0.0), axis=1, keepdims=True)
                row = row / pivot
                column = jnp.sum(jnp.where(wide_c == i, a, 0.0), axis=1, keepdims=True)
                gj[...] = jnp.where(wide_r == i, row, a - column * row)
                return 0

            lax.fori_loop(0, states, eliminate, 0)
            put(gj[:, 2 * LANES : 3 * LANES])

    late = pltpu.make_async_copy(inc, inc_ref, done.at[2])
    late.start()
    for copy in early:
        copy.wait()
    late.wait()


def shards(state_anom, radiance_anom, inv_noise, innovation, valid_count):
    profiles, local_members, states = state_anom.shape
    slab_width = radiance_anom.shape[2]
    mem = lax.axis_size("mem")
    chan = lax.axis_size("chan")
    members_all = local_members * mem
    f32 = jnp.float32
    both = pl.pallas_call(
        join_kernel,
        out_shape=jax.ShapeDtypeStruct((profiles, local_members, slab_width + 2 * LANES), jnp.bfloat16),
        in_specs=[pl.BlockSpec(memory_space=pltpu.HBM)] * 2,
        out_specs=pl.BlockSpec(memory_space=pltpu.HBM),
        scratch_shapes=[
            pltpu.VMEM((profiles, local_members, slab_width + 2 * LANES), jnp.bfloat16),
            pltpu.VMEM((profiles, local_members, states), jnp.bfloat16),
            pltpu.SemaphoreType.DMA((PIECES + 1,)),
            pltpu.SemaphoreType.DMA((PIECES,)),
        ],
        name="join",
    )(radiance_anom, state_anom)
    own = lax.all_to_all(both, "mem", split_axis=0, concat_axis=1, tiled=True)
    prof = lax.axis_index("mem")
    own_count = lax.dynamic_slice_in_dim(valid_count, prof, 1, 0)
    slots = lax.axis_index("chan") * slab_width + jnp.arange(slab_width, dtype=jnp.int32)
    weight = jnp.where(slots[None, :] < own_count[:, None], inv_noise[None, :], 0.0)
    innov = lax.dynamic_slice_in_dim(innovation, prof, 1, 0)
    part = pl.pallas_call(
        functools.partial(slab_kernel, states, members_all),
        out_shape=jax.ShapeDtypeStruct((PACKED, LANES), f32),
        in_specs=[pl.BlockSpec(memory_space=pltpu.VMEM)] * 3,
        out_specs=pl.BlockSpec(memory_space=pltpu.VMEM),
        compiler_params=pltpu.CompilerParams(vmem_limit_bytes=24 * 2**20),
        name="slab",
    )(own[0], weight, innov)
    parts = [part] + [
        lax.ppermute(part, "chan", [(j, (j + k) % chan) for j in range(chan)]) for k in (2, 1, 3)
    ]
    outs = [(states, 1, states), (1, states), (1, states)]
    square = pltpu.VMEM((LANES + 16, LANES), f32)
    info, grad, inc = pl.pallas_call(
        functools.partial(solve_kernel, states),
        out_shape=[jax.ShapeDtypeStruct(shape, f32) for shape in outs],
        in_specs=[pl.BlockSpec(memory_space=pltpu.VMEM)] * 4,
        out_specs=[pl.BlockSpec(memory_space=pltpu.HBM)] * 3,
        scratch_shapes=[pltpu.VMEM(shape, f32) for shape in outs]
        + [square] * 4
        + [pltpu.VMEM((LANES + 16, 3 * LANES), f32), pltpu.SemaphoreType.DMA((3,))],
        compiler_params=pltpu.CompilerParams(vmem_limit_bytes=8 * 2**20),
        name="solve",
    )(*parts)
    return (jnp.transpose(info, (1, 0, 2)), grad, inc)


def solution(mesh):
    in_specs = (P(None, "mem", None), P(None, "mem", "chan"), P("chan"), P(None, "chan"), P())
    out_specs = (P("mem", None, None), P("mem", None), P("mem", None))
    return jax.shard_map(shards, mesh=mesh, in_specs=in_specs, out_specs=out_specs, check_vma=False)
```

```python
import functools

import jax
import jax.numpy as jnp
from jax import lax
from jax.experimental import pallas as pl
from jax.experimental.pallas import tpu as pltpu
from jax.sharding import PartitionSpec as P

LANES = 128
TOL = 1e-5
FIRST_STEPS = 10
MORE_STEPS = 6
MORE_ROUNDS = 8
PACKED = 96


def places(rows):
    r = lax.broadcasted_iota(jnp.int32, (rows, LANES), 0)
    c = lax.broadcasted_iota(jnp.int32, (rows, LANES), 1)
    return r, c


SIZE_X, SIZE_Z, SIZE_C = 4, 8, 2
ACROSS = tuple((dx, dc) for dx in range(SIZE_X) for dc in range(SIZE_C))
NEAR = (2, -2, 1, -1, 0)
FAR = (4, 3, -3)
SENT = len(NEAR) - 1 + len(ACROSS) - 1


def partner(x, z, c):
    return (x % SIZE_X * SIZE_Z + z % SIZE_Z) * SIZE_C + c % SIZE_C


def spread_kernel(rad_ref, st_ref, *refs):
    outs, own, held, (st, arrived, left) = refs[:SENT], refs[SENT : SENT + 2], refs[SENT + 2 : -3], refs[-3:]
    width = rad_ref.shape[2]
    states = st_ref.shape[2]
    me = lax.axis_index("mem")
    x, z, c = me // (SIZE_Z * SIZE_C), me // SIZE_C % SIZE_Z, me % SIZE_C
    first = pltpu.make_async_copy(st_ref, st, arrived.at[SIZE_X * SIZE_Z * SIZE_C])
    first.start()
    near = held[: len(NEAR) - 1] + own[:1]
    far = own[1:] + held[len(NEAR) - 1 :]
    groups = [(near[i], [(k, dz, o) for k, o in enumerate(ACROSS)]) for i, dz in enumerate(NEAR)]
    groups += [(far[i], [(k, dz, o) for k, dz in enumerate(FAR)]) for i, o in enumerate(ACROSS)]
    groups.sort(key=lambda group: any(group[0] is ref for ref in own))
    copies, count = [], 0
    for ref, slots in groups:
        copies.append([])
        for k, dz, (dx, dc) in slots:
            p = lax.rem(x + dx, SIZE_X) * (SIZE_Z * SIZE_C) + lax.rem(z + dz + SIZE_Z, SIZE_Z) * SIZE_C + lax.rem(c + dc, SIZE_C)
            copy = pltpu.make_async_copy(rad_ref.at[p], ref.at[k, :, pl.ds(0, width)], arrived.at[count])
            copy.start()
            copies[-1].append((copy, k, p))
            count += 1
    first.wait()
    for (ref, _), group in zip(groups, copies):
        for _, k, p in group:
            ref[k, :, width : width + states] = st[p]
    away = []
    for (ref, _), group in zip(groups, copies):
        for copy, _, _ in group:
            copy.wait()
        for i, source in enumerate(held):
            if source is ref:
                away.append(pltpu.make_async_copy(ref, outs[i], left.at[i]))
                away[-1].start()
    for copy in away:
        copy.wait()


def swap_kernel(many, *refs):
    come, go = refs[:many], refs[many:]
    for i, ref in enumerate(come):
        for j, out in enumerate(go):
            out[i] = ref[j]


def in_vmem(kernel, outs, count, **more):
    return pl.pallas_call(
        kernel,
        out_shape=outs,
        in_specs=[pl.BlockSpec(memory_space=pltpu.VMEM)] * count,
        out_specs=[pl.BlockSpec(memory_space=pltpu.VMEM)] * len(outs),
        compiler_params=pltpu.CompilerParams(vmem_limit_bytes=20 * 2**20),
        **more,
    )


def moved(a, dx, dz, dc):
    pairs = [
        (partner(x, z, c), partner(x + dx, z + dz, c + dc))
        for x in range(SIZE_X)
        for z in range(SIZE_Z)
        for c in range(SIZE_C)
    ]
    return lax.ppermute(a, "mem", pairs)


def gathered(rad, st):
    members, width = rad.shape[1], rad.shape[2] + 2 * LANES
    tall = [jax.ShapeDtypeStruct((len(ACROSS), members, width), rad.dtype)]
    flat = [jax.ShapeDtypeStruct((len(FAR), members, width), rad.dtype)]
    five = [jax.ShapeDtypeStruct((len(NEAR), members, width), rad.dtype)]
    sent = tall * (len(NEAR) - 1) + flat * (len(ACROSS) - 1)
    own = tall + flat
    spread = pl.pallas_call(
        spread_kernel,
        out_shape=sent + [pltpu.VMEM(a.shape, a.dtype) for a in own],
        in_specs=[pl.BlockSpec(memory_space=pltpu.HBM)] * 2,
        out_specs=[pl.BlockSpec(memory_space=pltpu.HBM)] * SENT + [pl.BlockSpec(memory_space=pltpu.VMEM)] * 2,
        scratch_shapes=[pltpu.VMEM(a.shape, a.dtype) for a in sent]
        + [
            pltpu.VMEM(st.shape, st.dtype),
            pltpu.SemaphoreType.DMA((st.shape[0] + 1,)),
            pltpu.SemaphoreType.DMA((SENT,)),
        ],
        compiler_params=pltpu.CompilerParams(vmem_limit_bytes=59 * 10**6),
        name="spread",
    )(rad, st)
    near = spread[: len(NEAR) - 1] + spread[SENT : SENT + 1]
    far = spread[SENT + 1 :] + spread[len(NEAR) - 1 : SENT]
    near = [a if dz == 0 else moved(a, 0, dz, 0) for a, dz in zip(near, NEAR)]
    far = [a if o == (0, 0) else moved(a, o[0], 0, o[1]) for a, o in zip(far, ACROSS)]
    far = in_vmem(functools.partial(swap_kernel, len(ACROSS)), tall * len(FAR), len(ACROSS))(*far)
    far = [moved(a, 0, dz, 0) for a, dz in zip(far, FAR)]
    near = in_vmem(functools.partial(swap_kernel, len(NEAR)), five * len(ACROSS), len(NEAR))(*near)
    near = [a if o == (0, 0) else moved(a, o[0], 0, o[1]) for a, o in zip(near, ACROSS)]
    return far + near


def slab_kernel(states, members_all, *refs):
    parts, (weight_ref, innov_ref, out_ref, x_ref) = refs[:-4], refs[-4:]
    width = weight_ref.shape[1]
    at = 0
    for part in parts:
        rows = part.shape[0] * part.shape[1]
        x_ref[at : at + rows, :] = part[...].reshape(rows, part.shape[2])
        at += rows
    rad = x_ref[:, 0:width]
    st = x_ref[:, width : width + states]
    cross = lax.dot_general(st, rad, (((0,), (0,)), ((), ())), preferred_element_type=jnp.float32)
    root = jnp.sqrt(weight_ref[...])
    y = cross * (root * (1.0 / (members_all - 1)))
    y1 = y.astype(jnp.bfloat16)
    y2 = (y - y1.astype(jnp.float32)).astype(jnp.bfloat16)
    nt = (((1,), (1,)), ((), ()))
    main = lax.dot_general(y1, y1, nt, preferred_element_type=jnp.float32)
    side = lax.dot_general(y2, y1, nt, preferred_element_type=jnp.float32)
    info = main + (side + side.T)
    grad = jnp.sum(y * (root * innov_ref[...]), axis=1, keepdims=True)
    r = lax.broadcasted_iota(jnp.int32, info.shape, 0)
    c = lax.broadcasted_iota(jnp.int32, info.shape, 1)
    grad_row = jnp.sum(jnp.where(r == c, grad, 0.0), axis=0, keepdims=True)
    rest = states - LANES
    half = LANES // 2
    other = pltpu.roll(info[half:LANES, 0:LANES], half, 1)
    r, c = places(half)
    out_ref[0:half, :] = jnp.where(c < r, other, info[0:half, 0:LANES])
    out_ref[half:, :] = jnp.zeros((PACKED - half, LANES), jnp.float32)
    out_ref[half : half + rest, :] = info[LANES:states, 0:LANES]
    out_ref[half + rest : half + rest + 1, :] = grad_row[:, 0:LANES]
    out_ref[half + rest + 1 : half + rest + 2, :] = jnp.sum(jnp.where(r == c, other, 0.0), axis=0, keepdims=True)
    out_ref[half + 16 : half + 16 + rest, 0:rest] = info[LANES:states, LANES:states]
    out_ref[half + 16 + rest : half + 17 + rest, 0:rest] = grad_row[:, LANES:states]


def solve_kernel(
    states, a_ref, b_ref, c_ref, d_ref, info_ref, grad_ref, inc_ref, info, grad, inc, left, right, x_ref, r_ref, gj, done
):
    rest = states - LANES
    rows = LANES + 16
    half = LANES // 2
    total = (a_ref[...] + b_ref[...]) + (c_ref[...] + d_ref[...])
    r, c = places(half)
    ra, ca = places(LANES)
    last = jnp.where(ca[0:1] < half, total[half + rest + 1 : half + rest + 2, :], 0.0)
    lower = jnp.where(c < r, total[0:half], 0.0) + jnp.where(c == r, last, 0.0)
    part = jnp.concatenate([jnp.where(c < r, 0.0, total[0:half]), pltpu.roll(lower, half, 1)], axis=0)
    square = jnp.where(ra == ca, part, part + part.T)
    r, c = places(16)
    low = jnp.where(r < rest, total[half : half + 16, :], 0.0)
    corner = jnp.where((r < rest) & (c < rest), total[half + 16 : half + 32, :], 0.0)
    g0 = total[half + rest : half + rest + 1, :]
    g1 = total[half + 16 + rest : half + 17 + rest, :]
    upper = jnp.concatenate([low, jnp.zeros((LANES - 16, LANES), jnp.float32)], axis=0).T
    info[:, 0, 0:LANES] = jnp.concatenate([square, low[0:rest]], axis=0)
    info[:, 0, LANES:states] = jnp.concatenate([upper[:, 0:rest], corner[0:rest, 0:rest]], axis=0)
    grad[:, 0:LANES] = g0
    grad[:, LANES:states] = g1[:, 0:rest]
    eye = (ra == ca).astype(jnp.float32)
    eye_low = (r == c).astype(jnp.float32)
    left[0:LANES, :] = square + eye
    left[LANES:rows, :] = low
    right[0:LANES, :] = upper
    right[LANES:rows, :] = corner + eye_low
    early = (
        pltpu.make_async_copy(info, info_ref, done.at[0]),
        pltpu.make_async_copy(grad, grad_ref, done.at[1]),
    )
    for copy in early:
        copy.start()

    def to_rows(v):
        return (
            jnp.sum(v[0:LANES] * eye, axis=0, keepdims=True),
            jnp.sum(v[LANES:rows] * eye_low, axis=0, keepdims=True),
        )

    def times(v):
        v0, v1 = to_rows(v)
        return jnp.broadcast_to(jnp.sum(left[...] * v0 + right[...] * v1, axis=1, keepdims=True), (rows, LANES))

    def dot(u, v):
        return jnp.sum(u * v, axis=0, keepdims=True)

    def ratio(num, den):
        return jnp.where(den > 0.0, num / jnp.where(den > 0.0, den, 1.0), 0.0)

    def steps(n, x, res, p, s, gamma, alpha):
        for _ in range(n):
            w = times(res)
            new = dot(res, res)
            delta = dot(res, w)
            if gamma is None:
                alpha = ratio(new, delta)
                p, s = res, w
            else:
                beta = ratio(new, gamma)
                alpha = ratio(new, delta - beta * ratio(new, alpha))
                p = res + beta * p
                s = w + beta * s
            x = x + alpha * p
            res = res - alpha * s
            gamma = new
        return x, res

    col = jnp.concatenate(
        [
            jnp.broadcast_to(jnp.sum(eye * g0, axis=1, keepdims=True), (LANES, LANES)),
            jnp.broadcast_to(jnp.sum(jnp.where(c < rest, eye_low * g1, 0.0), axis=1, keepdims=True), (16, LANES)),
        ],
        axis=0,
    )

    def put(x):
        x0, x1 = to_rows(x)
        inc[:, 0:LANES] = x0
        inc[:, LANES:states] = x1[:, 0:rest]

    def open_after(x):
        res = col - times(x)
        bad = jnp.logical_not(dot(res, res) <= (TOL * TOL) * dot(x, x))
        return jnp.max(bad[:, 0:1].astype(jnp.int32)), res

    x, _ = steps(FIRST_STEPS, jnp.zeros_like(col), col, None, None, None, None)
    put(x)
    still, res = open_after(x)

    @pl.when(still > 0)
    def _():
        x_ref[...] = x
        r_ref[...] = res

        def more(state):
            k, _ = state
            x, _ = steps(MORE_STEPS, x_ref[...], r_ref[...], None, None, None, None)
            still, res = open_after(x)
            x_ref[...] = x
            r_ref[...] = res
            return k + 1, still

        _, open_still = lax.while_loop(
            lambda s: (s[0] < MORE_ROUNDS) & (s[1] > 0), more, (jnp.int32(0), jnp.int32(1))
        )
        put(x_ref[...])

        @pl.when(open_still > 0)
        def _():
            wide_r = lax.broadcasted_iota(jnp.int32, (rows, 3 * LANES), 0)
            wide_c = lax.broadcasted_iota(jnp.int32, (rows, 3 * LANES), 1)
            gj[:, 0:LANES] = left[...]
            gj[:, LANES : 2 * LANES] = right[...]
            gj[:, 2 * LANES : 3 * LANES] = col

            def eliminate(i, _):
                a = gj[...]
                row = jnp.sum(jnp.where(wide_r == i, a, 0.0), axis=0, keepdims=True)
                lane = lax.broadcasted_iota(jnp.int32, row.shape, 1)
                pivot = jnp.sum(jnp.where(lane == i, row, 0.0), axis=1, keepdims=True)
                row = row / pivot
                column = jnp.sum(jnp.where(wide_c == i, a, 0.0), axis=1, keepdims=True)
                gj[...] = jnp.where(wide_r == i, row, a - column * row)
                return 0

            lax.fori_loop(0, states, eliminate, 0)
            put(gj[:, 2 * LANES : 3 * LANES])

    late = pltpu.make_async_copy(inc, inc_ref, done.at[2])
    late.start()
    for copy in early:
        copy.wait()
    late.wait()


def shards(state_anom, radiance_anom, inv_noise, innovation, valid_count):
    _, local_members, states = state_anom.shape
    slab_width = radiance_anom.shape[2]
    mem = lax.axis_size("mem")
    chan = lax.axis_size("chan")
    members_all = local_members * mem
    f32 = jnp.float32
    blocks = gathered(radiance_anom, state_anom)
    prof = lax.axis_index("mem")
    own_count = lax.dynamic_slice_in_dim(valid_count, prof, 1, 0)
    slots = lax.axis_index("chan") * slab_width + jnp.arange(slab_width, dtype=jnp.int32)
    weight = jnp.where(slots[None, :] < own_count[:, None], inv_noise[None, :], 0.0)
    innov = lax.dynamic_slice_in_dim(innovation, prof, 1, 0)
    part = pl.pallas_call(
        functools.partial(slab_kernel, states, members_all),
        out_shape=jax.ShapeDtypeStruct((PACKED, LANES), f32),
        in_specs=[pl.BlockSpec(memory_space=pltpu.VMEM)] * (len(blocks) + 2),
        out_specs=pl.BlockSpec(memory_space=pltpu.VMEM),
        scratch_shapes=[pltpu.VMEM((members_all, slab_width + 2 * LANES), jnp.bfloat16)],
        compiler_params=pltpu.CompilerParams(vmem_limit_bytes=24 * 2**20),
        name="slab",
    )(*blocks, weight, innov)
    parts = [part] + [
        lax.ppermute(part, "chan", [(j, (j + k) % chan) for j in range(chan)]) for k in (2, 1, 3)
    ]
    outs = [(states, 1, states), (1, states), (1, states)]
    square = pltpu.VMEM((LANES + 16, LANES), f32)
    info, grad, inc = pl.pallas_call(
        functools.partial(solve_kernel, states),
        out_shape=[jax.ShapeDtypeStruct(shape, f32) for shape in outs],
        in_specs=[pl.BlockSpec(memory_space=pltpu.VMEM)] * 4,
        out_specs=[pl.BlockSpec(memory_space=pltpu.HBM)] * 3,
        scratch_shapes=[pltpu.VMEM(shape, f32) for shape in outs]
        + [square] * 4
        + [pltpu.VMEM((LANES + 16, 3 * LANES), f32), pltpu.SemaphoreType.DMA((3,))],
        compiler_params=pltpu.CompilerParams(vmem_limit_bytes=8 * 2**20),
        name="solve",
    )(*parts)
    return (jnp.transpose(info, (1, 0, 2)), grad, inc)


def solution(mesh):
    in_specs = (P(None, "mem", None), P(None, "mem", "chan"), P("chan"), P(None, "chan"), P())
    out_specs = (P("mem", None, None), P("mem", None), P("mem", None))
    return jax.shard_map(shards, mesh=mesh, in_specs=in_specs, out_specs=out_specs, check_vma=False)
```

```python
import functools

import jax
import jax.numpy as jnp
from jax import lax
from jax.experimental import pallas as pl
from jax.experimental.pallas import tpu as pltpu
from jax.sharding import PartitionSpec as P

LANES = 128
TOL = 2e-5
FIRST_STEPS = 11
MORE_STEPS = 6
MORE_ROUNDS = 8
PACKED = 96


def places(rows):
    r = lax.broadcasted_iota(jnp.int32, (rows, LANES), 0)
    c = lax.broadcasted_iota(jnp.int32, (rows, LANES), 1)
    return r, c


SIZE_X, SIZE_Z, SIZE_C = 4, 8, 2
ACROSS = ((0, 0), (2, 0), (2, 1), (1, 0), (3, 0), (1, 1), (3, 1), (0, 1))
NEAR = (2, -2, 1, -1, 0)
FAR = (4, 3, -3)
SENT = len(NEAR) - 1 + len(ACROSS) - 1


def partner(x, z, c):
    return (x % SIZE_X * SIZE_Z + z % SIZE_Z) * SIZE_C + c % SIZE_C


def slot_of(me, dx, dz, dc):
    x, z, c = me // (SIZE_Z * SIZE_C), me // SIZE_C % SIZE_Z, me % SIZE_C
    across = lax.rem(x + dx, SIZE_X) * (SIZE_Z * SIZE_C) + lax.rem(c + dc, SIZE_C)
    return across + lax.rem(z + dz + SIZE_Z, SIZE_Z) * SIZE_C


def spread_kernel(rad_ref, st_ref, *refs):
    outs, own, held, (st, arrived, left) = refs[:SENT], refs[SENT : SENT + 2], refs[SENT + 2 : -3], refs[-3:]
    width = rad_ref.shape[2]
    states = st_ref.shape[2]
    me = lax.axis_index("mem")
    first = pltpu.make_async_copy(st_ref, st, arrived.at[SIZE_X * SIZE_Z * SIZE_C])
    first.start()
    near = held[: len(NEAR) - 1] + own[:1]
    far = own[1:] + held[len(NEAR) - 1 :]
    groups = [(near[i], [(k, dz, o) for k, o in enumerate(ACROSS)]) for i, dz in enumerate(NEAR)]
    groups += [(far[i], [(k, dz, o) for k, dz in enumerate(FAR)]) for i, o in enumerate(ACROSS)]
    groups.sort(key=lambda group: any(group[0] is ref for ref in own))
    copies, count = [], 0
    for ref, slots in groups:
        copies.append([])
        for k, dz, (dx, dc) in slots:
            p = slot_of(me, dx, dz, dc)
            copy = pltpu.make_async_copy(rad_ref.at[p], ref.at[k, :, pl.ds(0, width)], arrived.at[count])
            copy.start()
            copies[-1].append((copy, k, p))
            count += 1
    first.wait()
    for (ref, _), group in zip(groups, copies):
        for _, k, p in group if any(ref is each for each in near) else ():
            ref[k, :, width : width + states] = st[p]
    away = []
    for (ref, _), group in zip(groups, copies):
        for copy, _, _ in group:
            copy.wait()
        for i, source in enumerate(held):
            if source is ref:
                away.append(pltpu.make_async_copy(ref, outs[i], left.at[i]))
                away[-1].start()
    for copy in away:
        copy.wait()


def pack_kernel(st_ref, *outs):
    me = lax.axis_index("mem")
    for dz, out in zip(FAR, outs):
        ends = []
        for o, (dx, dc) in enumerate(ACROSS):
            p = slot_of(me, dx, dz, dc)
            out[o] = st_ref[p, :, 0:LANES]
            ends.append(st_ref[p, :, LANES:].astype(jnp.float32))
        rest = st_ref.shape[2] - LANES
        ends.append(jnp.zeros((ends[0].shape[0], LANES - rest * len(ACROSS)), jnp.float32))
        out[len(ACROSS)] = jnp.concatenate(ends, axis=1).astype(out.dtype)


def swap_kernel(many, *refs):
    come, go = refs[:many], refs[many:]
    for i, ref in enumerate(come):
        for j, out in enumerate(go):
            out[i] = ref[j]


def swap_both_kernel(states, *refs):
    near, packed, outs = refs[: len(NEAR)], refs[len(NEAR) : len(NEAR) + len(FAR)], refs[len(NEAR) + len(FAR) :]
    base = near[0].shape[2]
    rest = states - LANES
    for i, ref in enumerate(near):
        for o, out in enumerate(outs):
            out[i, :, 0:base] = ref[o]
    for d, ref in enumerate(packed):
        ends = ref[len(outs)].astype(jnp.float32)
        for o, out in enumerate(outs):
            out[d, :, base : base + LANES] = ref[o]
            out[d, :, base + LANES : base + states] = ends[:, o * rest : (o + 1) * rest].astype(out.dtype)


def in_vmem(kernel, outs, count, **more):
    return pl.pallas_call(
        kernel,
        out_shape=outs,
        in_specs=[pl.BlockSpec(memory_space=pltpu.VMEM)] * count,
        out_specs=[pl.BlockSpec(memory_space=pltpu.VMEM)] * len(outs),
        compiler_params=pltpu.CompilerParams(vmem_limit_bytes=20 * 2**20),
        **more,
    )


def moved(a, dx, dz, dc):
    pairs = [
        (partner(x, z, c), partner(x + dx, z + dz, c + dc))
        for x in range(SIZE_X)
        for z in range(SIZE_Z)
        for c in range(SIZE_C)
    ]
    return lax.ppermute(a, "mem", pairs)


def gathered(rad, st):
    members, width = rad.shape[1], rad.shape[2]
    wide = width + 2 * LANES
    shape = lambda rows, lanes: [jax.ShapeDtypeStruct((rows, members, lanes), rad.dtype)]
    tall = shape(len(ACROSS), width)
    flat = shape(len(FAR), width)
    sent = shape(len(ACROSS), wide) * (len(NEAR) - 1) + flat * (len(ACROSS) - 1)
    spread = pl.pallas_call(
        spread_kernel,
        out_shape=sent + [pltpu.VMEM(a.shape, a.dtype) for a in shape(len(ACROSS), wide) + flat],
        in_specs=[pl.BlockSpec(memory_space=pltpu.HBM)] * 2,
        out_specs=[pl.BlockSpec(memory_space=pltpu.HBM)] * SENT + [pl.BlockSpec(memory_space=pltpu.VMEM)] * 2,
        scratch_shapes=[pltpu.VMEM(a.shape, a.dtype) for a in sent]
        + [
            pltpu.VMEM(st.shape, st.dtype),
            pltpu.SemaphoreType.DMA((st.shape[0] + 1,)),
            pltpu.SemaphoreType.DMA((SENT,)),
        ],
        compiler_params=pltpu.CompilerParams(vmem_limit_bytes=59 * 10**6),
        name="spread",
    )(rad, st)
    near = spread[: len(NEAR) - 1] + spread[SENT : SENT + 1]
    far = spread[SENT + 1 :] + spread[len(NEAR) - 1 : SENT]
    near = [a if dz == 0 else moved(a, 0, dz, 0) for a, dz in zip(near, NEAR)]
    far = [a if o == (0, 0) else moved(a, o[0], 0, o[1]) for a, o in zip(far, ACROSS)]
    packed = in_vmem(pack_kernel, shape(len(ACROSS) + 1, LANES) * len(FAR), 1)(st)
    packed = [moved(a, 0, dz, 0) for a, dz in zip(packed, FAR)]
    far = in_vmem(functools.partial(swap_kernel, len(ACROSS)), tall * len(FAR), len(ACROSS))(*far)
    far = [moved(a, 0, dz, 0) for a, dz in zip(far, FAR)]
    both = shape(len(NEAR), wide + 2 * LANES) * len(ACROSS)
    swap_both = in_vmem(functools.partial(swap_both_kernel, st.shape[2]), both, len(NEAR) + len(FAR))
    near = swap_both(*near, *packed)
    near = [a if o == (0, 0) else moved(a, o[0], 0, o[1]) for a, o in zip(near, ACROSS)]
    return far + near


def slab_kernel(states, members_all, *refs):
    parts, (weight_ref, innov_ref, out_ref, x_ref) = refs[:-4], refs[-4:]
    width = weight_ref.shape[1]
    far, near = parts[: len(FAR)], parts[len(FAR) :]
    members = far[0].shape[1]
    block = members * len(NEAR)
    above = members * len(ACROSS) * len(FAR)
    for k, part in enumerate(far):
        x_ref[k * members * len(ACROSS) : (k + 1) * members * len(ACROSS), 0:width] = part[...].reshape(-1, width)
    for o, part in enumerate(near):
        x_ref[above + o * block : above + (o + 1) * block, :] = part[:, :, 0 : x_ref.shape[1]].reshape(block, -1)
        for k in range(len(FAR)):
            row = (k * len(ACROSS) + o) * members
            base = width + 2 * LANES
            x_ref[row : row + members, width : width + states] = part[k, :, base : base + states]
    rad = x_ref[:, 0:width]
    st = x_ref[:, width : width + states]
    cross = lax.dot_general(st, rad, (((0,), (0,)), ((), ())), preferred_element_type=jnp.float32)
    root = jnp.sqrt(weight_ref[...])
    y = cross * (root * (1.0 / (members_all - 1)))
    y1 = y.astype(jnp.bfloat16)
    y2 = (y - y1.astype(jnp.float32)).astype(jnp.bfloat16)
    nt = (((1,), (1,)), ((), ()))
    main = lax.dot_general(y1, y1, nt, preferred_element_type=jnp.float32)
    side = lax.dot_general(y2, y1, nt, preferred_element_type=jnp.float32)
    info = main + (side + side.T)
    grad = jnp.sum(y * (root * innov_ref[...]), axis=1, keepdims=True)
    r = lax.broadcasted_iota(jnp.int32, info.shape, 0)
    c = lax.broadcasted_iota(jnp.int32, info.shape, 1)
    grad_row = jnp.sum(jnp.where(r == c, grad, 0.0), axis=0, keepdims=True)
    rest = states - LANES
    half = LANES // 2
    other = pltpu.roll(info[half:LANES, 0:LANES], half, 1)
    r, c = places(half)
    out_ref[0:half, :] = jnp.where(c < r, other, info[0:half, 0:LANES])
    out_ref[half:, :] = jnp.zeros((PACKED - half, LANES), jnp.float32)
    out_ref[half : half + rest, :] = info[LANES:states, 0:LANES]
    out_ref[half + rest : half + rest + 1, :] = grad_row[:, 0:LANES]
    out_ref[half + rest + 1 : half + rest + 2, :] = jnp.sum(jnp.where(r == c, other, 0.0), axis=0, keepdims=True)
    out_ref[half + 16 : half + 16 + rest, 0:rest] = info[LANES:states, LANES:states]
    out_ref[half + 16 + rest : half + 17 + rest, 0:rest] = grad_row[:, LANES:states]


def solve_kernel(
    states, a_ref, b_ref, c_ref, d_ref, info_ref, grad_ref, inc_ref, info, grad, inc, left, right, x_ref, r_ref, gj, done
):
    rest = states - LANES
    rows = LANES + 16
    half = LANES // 2
    total = (a_ref[...] + b_ref[...]) + (c_ref[...] + d_ref[...])
    r, c = places(half)
    ra, ca = places(LANES)
    last = jnp.where(ca[0:1] < half, total[half + rest + 1 : half + rest + 2, :], 0.0)
    lower = jnp.where(c < r, total[0:half], 0.0) + jnp.where(c == r, last, 0.0)
    part = jnp.concatenate([jnp.where(c < r, 0.0, total[0:half]), pltpu.roll(lower, half, 1)], axis=0)
    square = jnp.where(ra == ca, part, part + part.T)
    r, c = places(16)
    low = jnp.where(r < rest, total[half : half + 16, :], 0.0)
    corner = jnp.where((r < rest) & (c < rest), total[half + 16 : half + 32, :], 0.0)
    g0 = total[half + rest : half + rest + 1, :]
    g1 = total[half + 16 + rest : half + 17 + rest, :]
    upper = jnp.concatenate([low, jnp.zeros((LANES - 16, LANES), jnp.float32)], axis=0).T
    info[:, 0, 0:LANES] = jnp.concatenate([square, low[0:rest]], axis=0)
    info[:, 0, LANES:states] = jnp.concatenate([upper[:, 0:rest], corner[0:rest, 0:rest]], axis=0)
    grad[:, 0:LANES] = g0
    grad[:, LANES:states] = g1[:, 0:rest]
    eye = (ra == ca).astype(jnp.float32)
    eye_low = (r == c).astype(jnp.float32)
    left[0:LANES, :] = square + eye
    left[LANES:rows, :] = low
    right[0:LANES, :] = upper
    right[LANES:rows, :] = corner + eye_low
    early = (
        pltpu.make_async_copy(info, info_ref, done.at[0]),
        pltpu.make_async_copy(grad, grad_ref, done.at[1]),
    )
    for copy in early:
        copy.start()

    def to_rows(v):
        return (
            jnp.sum(v[0:LANES] * eye, axis=0, keepdims=True),
            jnp.sum(v[LANES:rows] * eye_low, axis=0, keepdims=True),
        )

    def times(v):
        v0, v1 = to_rows(v)
        return jnp.broadcast_to(jnp.sum(left[...] * v0 + right[...] * v1, axis=1, keepdims=True), (rows, LANES))

    def dot(u, v):
        return jnp.sum(u * v, axis=0, keepdims=True)

    def ratio(num, den):
        return jnp.where(den > 0.0, num / jnp.where(den > 0.0, den, 1.0), 0.0)

    def steps(n, x, res, p, s, gamma, alpha):
        for _ in range(n):
            w = times(res)
            new = dot(res, res)
            delta = dot(res, w)
            if gamma is None:
                alpha = ratio(new, delta)
                p, s = res, w
            else:
                beta = ratio(new, gamma)
                alpha = ratio(new, delta - beta * ratio(new, alpha))
                p = res + beta * p
                s = w + beta * s
            x = x + alpha * p
            res = res - alpha * s
            gamma = new
        return x, res

    col = jnp.concatenate(
        [
            jnp.broadcast_to(jnp.sum(eye * g0, axis=1, keepdims=True), (LANES, LANES)),
            jnp.broadcast_to(jnp.sum(jnp.where(c < rest, eye_low * g1, 0.0), axis=1, keepdims=True), (16, LANES)),
        ],
        axis=0,
    )

    def put(x):
        x0, x1 = to_rows(x)
        inc[:, 0:LANES] = x0
        inc[:, LANES:states] = x1[:, 0:rest]

    def open_after(x):
        res = col - times(x)
        bad = jnp.logical_not(dot(res, res) <= (TOL * TOL) * dot(x, x))
        return jnp.max(bad[:, 0:1].astype(jnp.int32)), res

    x, _ = steps(FIRST_STEPS, jnp.zeros_like(col), col, None, None, None, None)
    put(x)
    still, res = open_after(x)

    @pl.when(still > 0)
    def _():
        x_ref[...] = x
        r_ref[...] = res

        def more(state):
            k, _ = state
            x, _ = steps(MORE_STEPS, x_ref[...], r_ref[...], None, None, None, None)
            still, res = open_after(x)
            x_ref[...] = x
            r_ref[...] = res
            return k + 1, still

        _, open_still = lax.while_loop(
            lambda s: (s[0] < MORE_ROUNDS) & (s[1] > 0), more, (jnp.int32(0), jnp.int32(1))
        )
        put(x_ref[...])

        @pl.when(open_still > 0)
        def _():
            wide_r = lax.broadcasted_iota(jnp.int32, (rows, 3 * LANES), 0)
            wide_c = lax.broadcasted_iota(jnp.int32, (rows, 3 * LANES), 1)
            gj[:, 0:LANES] = left[...]
            gj[:, LANES : 2 * LANES] = right[...]
            gj[:, 2 * LANES : 3 * LANES] = col

            def eliminate(i, _):
                a = gj[...]
                row = jnp.sum(jnp.where(wide_r == i, a, 0.0), axis=0, keepdims=True)
                lane = lax.broadcasted_iota(jnp.int32, row.shape, 1)
                pivot = jnp.sum(jnp.where(lane == i, row, 0.0), axis=1, keepdims=True)
                row = row / pivot
                column = jnp.sum(jnp.where(wide_c == i, a, 0.0), axis=1, keepdims=True)
                gj[...] = jnp.where(wide_r == i, row, a - column * row)
                return 0

            lax.fori_loop(0, states, eliminate, 0)
            put(gj[:, 2 * LANES : 3 * LANES])

    late = pltpu.make_async_copy(inc, inc_ref, done.at[2])
    late.start()
    for copy in early:
        copy.wait()
    late.wait()


def shards(state_anom, radiance_anom, inv_noise, innovation, valid_count):
    _, local_members, states = state_anom.shape
    slab_width = radiance_anom.shape[2]
    mem = lax.axis_size("mem")
    chan = lax.axis_size("chan")
    members_all = local_members * mem
    f32 = jnp.float32
    blocks = gathered(radiance_anom, state_anom)
    prof = lax.axis_index("mem")
    own_count = lax.dynamic_slice_in_dim(valid_count, prof, 1, 0)
    slots = lax.axis_index("chan") * slab_width + jnp.arange(slab_width, dtype=jnp.int32)
    weight = jnp.where(slots[None, :] < own_count[:, None], inv_noise[None, :], 0.0)
    innov = lax.dynamic_slice_in_dim(innovation, prof, 1, 0)
    part = pl.pallas_call(
        functools.partial(slab_kernel, states, members_all),
        out_shape=jax.ShapeDtypeStruct((PACKED, LANES), f32),
        in_specs=[pl.BlockSpec(memory_space=pltpu.VMEM)] * (len(blocks) + 2),
        out_specs=pl.BlockSpec(memory_space=pltpu.VMEM),
        scratch_shapes=[pltpu.VMEM((members_all, slab_width + 2 * LANES), jnp.bfloat16)],
        compiler_params=pltpu.CompilerParams(vmem_limit_bytes=24 * 2**20),
        name="slab",
    )(*blocks, weight, innov)
    parts = [part] + [
        lax.ppermute(part, "chan", [(j, (j + k) % chan) for j in range(chan)]) for k in (2, 1, 3)
    ]
    outs = [(states, 1, states), (1, states), (1, states)]
    square = pltpu.VMEM((LANES + 16, LANES), f32)
    info, grad, inc = pl.pallas_call(
        functools.partial(solve_kernel, states),
        out_shape=[jax.ShapeDtypeStruct(shape, f32) for shape in outs],
        in_specs=[pl.BlockSpec(memory_space=pltpu.VMEM)] * 4,
        out_specs=[pl.BlockSpec(memory_space=pltpu.HBM)] * 3,
        scratch_shapes=[pltpu.VMEM(shape, f32) for shape in outs]
        + [square] * 4
        + [pltpu.VMEM((LANES + 16, 3 * LANES), f32), pltpu.SemaphoreType.DMA((3,))],
        compiler_params=pltpu.CompilerParams(vmem_limit_bytes=8 * 2**20),
        name="solve",
    )(*parts)
    return (jnp.transpose(info, (1, 0, 2)), grad, inc)


def solution(mesh):
    in_specs = (P(None, "mem", None), P(None, "mem", "chan"), P("chan"), P(None, "chan"), P())
    out_specs = (P("mem", None, None), P("mem", None), P("mem", None))
    return jax.shard_map(shards, mesh=mesh, in_specs=in_specs, out_specs=out_specs, check_vma=False)
```

```python
import functools

import jax
import jax.numpy as jnp
from jax import lax
from jax.experimental import pallas as pl
from jax.experimental.pallas import tpu as pltpu
from jax.sharding import PartitionSpec as P

LANES = 128
TOL = 2e-5
FIRST_STEPS = 11
MORE_STEPS = 6
MORE_ROUNDS = 8
PACKED = 96


def places(rows):
    r = lax.broadcasted_iota(jnp.int32, (rows, LANES), 0)
    c = lax.broadcasted_iota(jnp.int32, (rows, LANES), 1)
    return r, c


SIZE_X, SIZE_Z, SIZE_C = 4, 8, 2
ACROSS = ((0, 0), (2, 0), (2, 1), (1, 0), (3, 0), (1, 1), (3, 1), (0, 1))
NEAR = (2, -2, 1, -1, 0)
FAR = (4, 3, -3)
SENT = len(NEAR) - 1 + len(ACROSS) - 1


def partner(x, z, c):
    return (x % SIZE_X * SIZE_Z + z % SIZE_Z) * SIZE_C + c % SIZE_C


def slot_of(me, dx, dz, dc):
    x, z, c = me // (SIZE_Z * SIZE_C), me // SIZE_C % SIZE_Z, me % SIZE_C
    across = lax.rem(x + dx, SIZE_X) * (SIZE_Z * SIZE_C) + lax.rem(c + dc, SIZE_C)
    return across + lax.rem(z + dz + SIZE_Z, SIZE_Z) * SIZE_C


def spread_kernel(rad_ref, st_ref, *refs):
    outs, own, held, (st, arrived, left) = refs[:SENT], refs[SENT : SENT + 2], refs[SENT + 2 : -3], refs[-3:]
    width = rad_ref.shape[2]
    states = st_ref.shape[2]
    me = lax.axis_index("mem")
    first = pltpu.make_async_copy(st_ref, st, arrived.at[SIZE_X * SIZE_Z * SIZE_C])
    first.start()
    near = held[: len(NEAR) - 1] + own[:1]
    far = own[1:] + held[len(NEAR) - 1 :]
    groups = [(near[i], [(k, dz, o) for k, o in enumerate(ACROSS)]) for i, dz in enumerate(NEAR)]
    groups += [(far[i], [(k, dz, o) for k, dz in enumerate(FAR)]) for i, o in enumerate(ACROSS)]
    groups.sort(key=lambda group: any(group[0] is ref for ref in own))
    copies, count = [], 0
    for ref, slots in groups:
        copies.append([])
        for k, dz, (dx, dc) in slots:
            p = slot_of(me, dx, dz, dc)
            copy = pltpu.make_async_copy(rad_ref.at[p], ref.at[k, :, pl.ds(0, width)], arrived.at[count])
            copy.start()
            copies[-1].append((copy, k, p))
            count += 1
    first.wait()
    for (ref, _), group in zip(groups, copies):
        for _, k, p in group if any(ref is each for each in near) else ():
            ref[k, :, width : width + states] = st[p]
    away = []
    for (ref, _), group in zip(groups, copies):
        for copy, _, _ in group:
            copy.wait()
        for i, source in enumerate(held):
            if source is ref:
                away.append(pltpu.make_async_copy(ref, outs[i], left.at[i]))
                away[-1].start()
    for copy in away:
        copy.wait()


def pack_kernel(st_ref, *outs):
    me = lax.axis_index("mem")
    for dz, out in zip(FAR, outs):
        ends = []
        for o, (dx, dc) in enumerate(ACROSS):
            p = slot_of(me, dx, dz, dc)
            out[o] = st_ref[p, :, 0:LANES]
            ends.append(st_ref[p, :, LANES:].astype(jnp.float32))
        rest = st_ref.shape[2] - LANES
        ends.append(jnp.zeros((ends[0].shape[0], LANES - rest * len(ACROSS)), jnp.float32))
        out[len(ACROSS)] = jnp.concatenate(ends, axis=1).astype(out.dtype)


def swap_kernel(many, *refs):
    come, go = refs[:many], refs[many:]
    for i, ref in enumerate(come):
        for j, out in enumerate(go):
            out[i] = ref[j]


def swap_both_kernel(states, *refs):
    near, packed, outs = refs[: len(NEAR)], refs[len(NEAR) : len(NEAR) + len(FAR)], refs[len(NEAR) + len(FAR) :]
    base = near[0].shape[2]
    rest = states - LANES
    for i, ref in enumerate(near):
        for o, out in enumerate(outs):
            out[i, :, 0:base] = ref[o]
    for d, ref in enumerate(packed):
        ends = ref[len(outs)].astype(jnp.float32)
        for o, out in enumerate(outs):
            out[d, :, base : base + LANES] = ref[o]
            out[d, :, base + LANES : base + states] = ends[:, o * rest : (o + 1) * rest].astype(out.dtype)


def in_vmem(kernel, outs, count, **more):
    return pl.pallas_call(
        kernel,
        out_shape=outs,
        in_specs=[pl.BlockSpec(memory_space=pltpu.VMEM)] * count,
        out_specs=[pl.BlockSpec(memory_space=pltpu.VMEM)] * len(outs),
        compiler_params=pltpu.CompilerParams(vmem_limit_bytes=20 * 2**20),
        **more,
    )


def moved(a, dx, dz, dc):
    pairs = [
        (partner(x, z, c), partner(x + dx, z + dz, c + dc))
        for x in range(SIZE_X)
        for z in range(SIZE_Z)
        for c in range(SIZE_C)
    ]
    return lax.ppermute(a, "mem", pairs)


def gathered(rad, st):
    members, width = rad.shape[1], rad.shape[2]
    wide = width + 2 * LANES
    shape = lambda rows, lanes: [jax.ShapeDtypeStruct((rows, members, lanes), rad.dtype)]
    tall = shape(len(ACROSS), width)
    flat = shape(len(FAR), width)
    sent = shape(len(ACROSS), wide) * (len(NEAR) - 1) + flat * (len(ACROSS) - 1)
    spread = pl.pallas_call(
        spread_kernel,
        out_shape=sent + [pltpu.VMEM(a.shape, a.dtype) for a in shape(len(ACROSS), wide) + flat],
        in_specs=[pl.BlockSpec(memory_space=pltpu.HBM)] * 2,
        out_specs=[pl.BlockSpec(memory_space=pltpu.HBM)] * SENT + [pl.BlockSpec(memory_space=pltpu.VMEM)] * 2,
        scratch_shapes=[pltpu.VMEM(a.shape, a.dtype) for a in sent]
        + [
            pltpu.VMEM(st.shape, st.dtype),
            pltpu.SemaphoreType.DMA((st.shape[0] + 1,)),
            pltpu.SemaphoreType.DMA((SENT,)),
        ],
        compiler_params=pltpu.CompilerParams(vmem_limit_bytes=59 * 10**6),
        name="spread",
    )(rad, st)
    near = spread[: len(NEAR) - 1] + spread[SENT : SENT + 1]
    far = spread[SENT + 1 :] + spread[len(NEAR) - 1 : SENT]
    near = [a if dz == 0 else moved(a, 0, dz, 0) for a, dz in zip(near, NEAR)]
    far = [a if o == (0, 0) else moved(a, o[0], 0, o[1]) for a, o in zip(far, ACROSS)]
    packed = in_vmem(pack_kernel, shape(len(ACROSS) + 1, LANES) * len(FAR), 1)(st)
    packed = [moved(a, 0, dz, 0) for a, dz in zip(packed, FAR)]
    far = in_vmem(functools.partial(swap_kernel, len(ACROSS)), tall * len(FAR), len(ACROSS))(*far)
    far = [moved(a, 0, dz, 0) for a, dz in zip(far, FAR)]
    both = shape(len(NEAR), wide + 2 * LANES) * len(ACROSS)
    swap_both = in_vmem(functools.partial(swap_both_kernel, st.shape[2]), both, len(NEAR) + len(FAR))
    near = swap_both(*near, *packed)
    near = [a if o == (0, 0) else moved(a, o[0], 0, o[1]) for a, o in zip(near, ACROSS)]
    rows = members * len(ACROSS)
    sums = in_vmem(
        functools.partial(early_kernel, st.shape[2]),
        [
            jax.ShapeDtypeStruct((rows * len(FAR), 2 * LANES), rad.dtype),
            jax.ShapeDtypeStruct((st.shape[2], width), jnp.float32),
        ],
        len(ACROSS),
        scratch_shapes=[pltpu.VMEM((rows * len(NEAR), wide), rad.dtype)],
    )(*near)
    return list(far) + list(sums)


def early_kernel(states, *refs):
    near, (far_ref, cross_ref, x_ref) = refs[:-3], refs[-3:]
    width = cross_ref.shape[1]
    wide = x_ref.shape[1]
    members = near[0].shape[1]
    block = members * len(NEAR)
    for o, part in enumerate(near):
        x_ref[o * block : (o + 1) * block, :] = part[:, :, 0:wide].reshape(block, wide)
        for k in range(len(FAR)):
            row = (k * len(ACROSS) + o) * members
            far_ref[row : row + members, 0:states] = part[k, :, wide : wide + states]
    tn = (((0,), (0,)), ((), ()))
    st = x_ref[:, width : width + states]
    cross_ref[...] = lax.dot_general(st, x_ref[:, 0:width], tn, preferred_element_type=jnp.float32)


def slab_kernel(states, members_all, *refs):
    far, (states_ref, cross_ref, weight_ref, innov_ref, out_ref, x_ref) = refs[:-6], refs[-6:]
    rows = far[0].shape[0] * far[0].shape[1]
    for k, part in enumerate(far):
        x_ref[k * rows : (k + 1) * rows, :] = part[...].reshape(rows, -1)
    tn = (((0,), (0,)), ((), ()))
    st = states_ref[:, 0:states]
    cross = cross_ref[...] + lax.dot_general(st, x_ref[...], tn, preferred_element_type=jnp.float32)
    root = jnp.sqrt(weight_ref[...])
    y = cross * (root * (1.0 / (members_all - 1)))
    y1 = y.astype(jnp.bfloat16)
    y2 = (y - y1.astype(jnp.float32)).astype(jnp.bfloat16)
    nt = (((1,), (1,)), ((), ()))
    main = lax.dot_general(y1, y1, nt, preferred_element_type=jnp.float32)
    side = lax.dot_general(y2, y1, nt, preferred_element_type=jnp.float32)
    info = main + (side + side.T)
    grad = jnp.sum(y * (root * innov_ref[...]), axis=1, keepdims=True)
    r = lax.broadcasted_iota(jnp.int32, info.shape, 0)
    c = lax.broadcasted_iota(jnp.int32, info.shape, 1)
    grad_row = jnp.sum(jnp.where(r == c, grad, 0.0), axis=0, keepdims=True)
    rest = states - LANES
    half = LANES // 2
    other = pltpu.roll(info[half:LANES, 0:LANES], half, 1)
    r, c = places(half)
    out_ref[0:half, :] = jnp.where(c < r, other, info[0:half, 0:LANES])
    out_ref[half:, :] = jnp.zeros((PACKED - half, LANES), jnp.float32)
    out_ref[half : half + rest, :] = info[LANES:states, 0:LANES]
    out_ref[half + rest : half + rest + 1, :] = grad_row[:, 0:LANES]
    out_ref[half + rest + 1 : half + rest + 2, :] = jnp.sum(jnp.where(r == c, other, 0.0), axis=0, keepdims=True)
    out_ref[half + 16 : half + 16 + rest, 0:rest] = info[LANES:states, LANES:states]
    out_ref[half + 16 + rest : half + 17 + rest, 0:rest] = grad_row[:, LANES:states]


def solve_kernel(
    states, a_ref, b_ref, c_ref, d_ref, info_ref, grad_ref, inc_ref, info, grad, inc, left, right, x_ref, r_ref, gj, done
):
    rest = states - LANES
    rows = LANES + 16
    half = LANES // 2
    total = (a_ref[...] + b_ref[...]) + (c_ref[...] + d_ref[...])
    r, c = places(half)
    ra, ca = places(LANES)
    last = jnp.where(ca[0:1] < half, total[half + rest + 1 : half + rest + 2, :], 0.0)
    lower = jnp.where(c < r, total[0:half], 0.0) + jnp.where(c == r, last, 0.0)
    part = jnp.concatenate([jnp.where(c < r, 0.0, total[0:half]), pltpu.roll(lower, half, 1)], axis=0)
    square = jnp.where(ra == ca, part, part + part.T)
    r, c = places(16)
    low = jnp.where(r < rest, total[half : half + 16, :], 0.0)
    corner = jnp.where((r < rest) & (c < rest), total[half + 16 : half + 32, :], 0.0)
    g0 = total[half + rest : half + rest + 1, :]
    g1 = total[half + 16 + rest : half + 17 + rest, :]
    upper = jnp.concatenate([low, jnp.zeros((LANES - 16, LANES), jnp.float32)], axis=0).T
    info[:, 0, 0:LANES] = jnp.concatenate([square, low[0:rest]], axis=0)
    info[:, 0, LANES:states] = jnp.concatenate([upper[:, 0:rest], corner[0:rest, 0:rest]], axis=0)
    grad[:, 0:LANES] = g0
    grad[:, LANES:states] = g1[:, 0:rest]
    eye = (ra == ca).astype(jnp.float32)
    eye_low = (r == c).astype(jnp.float32)
    left[0:LANES, :] = square + eye
    left[LANES:rows, :] = low
    right[0:LANES, :] = upper
    right[LANES:rows, :] = corner + eye_low
    early = (
        pltpu.make_async_copy(info, info_ref, done.at[0]),
        pltpu.make_async_copy(grad, grad_ref, done.at[1]),
    )
    for copy in early:
        copy.start()

    def to_rows(v):
        return (
            jnp.sum(v[0:LANES] * eye, axis=0, keepdims=True),
            jnp.sum(v[LANES:rows] * eye_low, axis=0, keepdims=True),
        )

    def times(v):
        v0, v1 = to_rows(v)
        return jnp.broadcast_to(jnp.sum(left[...] * v0 + right[...] * v1, axis=1, keepdims=True), (rows, LANES))

    def dot(u, v):
        return jnp.sum(u * v, axis=0, keepdims=True)

    def ratio(num, den):
        return jnp.where(den > 0.0, num / jnp.where(den > 0.0, den, 1.0), 0.0)

    def steps(n, x, res, p, s, gamma, alpha):
        for _ in range(n):
            w = times(res)
            new = dot(res, res)
            delta = dot(res, w)
            if gamma is None:
                alpha = ratio(new, delta)
                p, s = res, w
            else:
                beta = ratio(new, gamma)
                alpha = ratio(new, delta - beta * ratio(new, alpha))
                p = res + beta * p
                s = w + beta * s
            x = x + alpha * p
            res = res - alpha * s
            gamma = new
        return x, res

    col = jnp.concatenate(
        [
            jnp.broadcast_to(jnp.sum(eye * g0, axis=1, keepdims=True), (LANES, LANES)),
            jnp.broadcast_to(jnp.sum(jnp.where(c < rest, eye_low * g1, 0.0), axis=1, keepdims=True), (16, LANES)),
        ],
        axis=0,
    )

    def put(x):
        x0, x1 = to_rows(x)
        inc[:, 0:LANES] = x0
        inc[:, LANES:states] = x1[:, 0:rest]

    def open_after(x):
        res = col - times(x)
        bad = jnp.logical_not(dot(res, res) <= (TOL * TOL) * dot(x, x))
        return jnp.max(bad[:, 0:1].astype(jnp.int32)), res

    x, _ = steps(FIRST_STEPS, jnp.zeros_like(col), col, None, None, None, None)
    put(x)
    still, res = open_after(x)

    @pl.when(still > 0)
    def _():
        x_ref[...] = x
        r_ref[...] = res

        def more(state):
            k, _ = state
            x, _ = steps(MORE_STEPS, x_ref[...], r_ref[...], None, None, None, None)
            still, res = open_after(x)
            x_ref[...] = x
            r_ref[...] = res
            return k + 1, still

        _, open_still = lax.while_loop(
            lambda s: (s[0] < MORE_ROUNDS) & (s[1] > 0), more, (jnp.int32(0), jnp.int32(1))
        )
        put(x_ref[...])

        @pl.when(open_still > 0)
        def _():
            wide_r = lax.broadcasted_iota(jnp.int32, (rows, 3 * LANES), 0)
            wide_c = lax.broadcasted_iota(jnp.int32, (rows, 3 * LANES), 1)
            gj[:, 0:LANES] = left[...]
            gj[:, LANES : 2 * LANES] = right[...]
            gj[:, 2 * LANES : 3 * LANES] = col

            def eliminate(i, _):
                a = gj[...]
                row = jnp.sum(jnp.where(wide_r == i, a, 0.0), axis=0, keepdims=True)
                lane = lax.broadcasted_iota(jnp.int32, row.shape, 1)
                pivot = jnp.sum(jnp.where(lane == i, row, 0.0), axis=1, keepdims=True)
                row = row / pivot
                column = jnp.sum(jnp.where(wide_c == i, a, 0.0), axis=1, keepdims=True)
                gj[...] = jnp.where(wide_r == i, row, a - column * row)
                return 0

            lax.fori_loop(0, states, eliminate, 0)
            put(gj[:, 2 * LANES : 3 * LANES])

    late = pltpu.make_async_copy(inc, inc_ref, done.at[2])
    late.start()
    for copy in early:
        copy.wait()
    late.wait()


def shards(state_anom, radiance_anom, inv_noise, innovation, valid_count):
    _, local_members, states = state_anom.shape
    slab_width = radiance_anom.shape[2]
    mem = lax.axis_size("mem")
    chan = lax.axis_size("chan")
    members_all = local_members * mem
    f32 = jnp.float32
    blocks = gathered(radiance_anom, state_anom)
    prof = lax.axis_index("mem")
    own_count = lax.dynamic_slice_in_dim(valid_count, prof, 1, 0)
    slots = lax.axis_index("chan") * slab_width + jnp.arange(slab_width, dtype=jnp.int32)
    weight = jnp.where(slots[None, :] < own_count[:, None], inv_noise[None, :], 0.0)
    innov = lax.dynamic_slice_in_dim(innovation, prof, 1, 0)
    part = pl.pallas_call(
        functools.partial(slab_kernel, states, members_all),
        out_shape=jax.ShapeDtypeStruct((PACKED, LANES), f32),
        in_specs=[pl.BlockSpec(memory_space=pltpu.VMEM)] * (len(blocks) + 2),
        out_specs=pl.BlockSpec(memory_space=pltpu.VMEM),
        scratch_shapes=[pltpu.VMEM(blocks[-2].shape[:1] + (slab_width,), jnp.bfloat16)],
        compiler_params=pltpu.CompilerParams(vmem_limit_bytes=24 * 2**20),
        name="slab",
    )(*blocks, weight, innov)
    parts = [part] + [
        lax.ppermute(part, "chan", [(j, (j + k) % chan) for j in range(chan)]) for k in (2, 1, 3)
    ]
    outs = [(states, 1, states), (1, states), (1, states)]
    square = pltpu.VMEM((LANES + 16, LANES), f32)
    info, grad, inc = pl.pallas_call(
        functools.partial(solve_kernel, states),
        out_shape=[jax.ShapeDtypeStruct(shape, f32) for shape in outs],
        in_specs=[pl.BlockSpec(memory_space=pltpu.VMEM)] * 4,
        out_specs=[pl.BlockSpec(memory_space=pltpu.HBM)] * 3,
        scratch_shapes=[pltpu.VMEM(shape, f32) for shape in outs]
        + [square] * 4
        + [pltpu.VMEM((LANES + 16, 3 * LANES), f32), pltpu.SemaphoreType.DMA((3,))],
        compiler_params=pltpu.CompilerParams(vmem_limit_bytes=8 * 2**20),
        name="solve",
    )(*parts)
    return (jnp.transpose(info, (1, 0, 2)), grad, inc)


def solution(mesh):
    in_specs = (P(None, "mem", None), P(None, "mem", "chan"), P("chan"), P(None, "chan"), P())
    out_specs = (P("mem", None, None), P("mem", None), P("mem", None))
    return jax.shard_map(shards, mesh=mesh, in_specs=in_specs, out_specs=out_specs, check_vma=False)
```

```python
import functools

import jax
import jax.numpy as jnp
from jax import lax
from jax.experimental import pallas as pl
from jax.experimental.pallas import tpu as pltpu
from jax.sharding import PartitionSpec as P

LANES = 128
TOL = 3e-5
FIRST_STEPS = 10
MORE_STEPS = 6
MORE_ROUNDS = 8
PACKED = 96


def places(rows):
    r = lax.broadcasted_iota(jnp.int32, (rows, LANES), 0)
    c = lax.broadcasted_iota(jnp.int32, (rows, LANES), 1)
    return r, c


SIZE_X, SIZE_Z, SIZE_C = 4, 8, 2
ACROSS = ((0, 0), (2, 0), (2, 1), (1, 0), (3, 0), (1, 1), (3, 1), (0, 1))
NEAR = (2, -2, 1, -1, 0)
FAR = (4, 3, -3)
SENT = len(NEAR) - 1 + len(ACROSS) - 1


def partner(x, z, c):
    return (x % SIZE_X * SIZE_Z + z % SIZE_Z) * SIZE_C + c % SIZE_C


def slot_of(me, dx, dz, dc):
    x, z, c = me // (SIZE_Z * SIZE_C), me // SIZE_C % SIZE_Z, me % SIZE_C
    across = lax.rem(x + dx, SIZE_X) * (SIZE_Z * SIZE_C) + lax.rem(c + dc, SIZE_C)
    return across + lax.rem(z + dz + SIZE_Z, SIZE_Z) * SIZE_C


def spread_kernel(rad_ref, st_ref, *refs):
    outs, own, held, (st, arrived, left) = refs[:SENT], refs[SENT : SENT + 2], refs[SENT + 2 : -3], refs[-3:]
    width = rad_ref.shape[2]
    states = st_ref.shape[2]
    me = lax.axis_index("mem")
    first = pltpu.make_async_copy(st_ref, st, arrived.at[SIZE_X * SIZE_Z * SIZE_C])
    first.start()
    near = held[: len(NEAR) - 1] + own[:1]
    far = own[1:] + held[len(NEAR) - 1 :]
    groups = [(near[i], [(k, dz, o) for k, o in enumerate(ACROSS)]) for i, dz in enumerate(NEAR)]
    groups += [(far[i], [(k, dz, o) for k, dz in enumerate(FAR)]) for i, o in enumerate(ACROSS)]
    groups.sort(key=lambda group: any(group[0] is ref for ref in own))
    copies, count = [], 0
    for ref, slots in groups:
        copies.append([])
        for k, dz, (dx, dc) in slots:
            p = slot_of(me, dx, dz, dc)
            copy = pltpu.make_async_copy(rad_ref.at[p], ref.at[k, :, pl.ds(0, width)], arrived.at[count])
            copy.start()
            copies[-1].append((copy, k, p))
            count += 1
    first.wait()
    for (ref, _), group in zip(groups, copies):
        for _, k, p in group if any(ref is each for each in near) else ():
            ref[k, :, width : width + states] = st[p]
    away = []
    for (ref, _), group in zip(groups, copies):
        for copy, _, _ in group:
            copy.wait()
        for i, source in enumerate(held):
            if source is ref:
                away.append(pltpu.make_async_copy(ref, outs[i], left.at[i]))
                away[-1].start()
    for copy in away:
        copy.wait()


def pack_kernel(st_ref, *outs):
    me = lax.axis_index("mem")
    for dz, out in zip(FAR, outs):
        ends = []
        for o, (dx, dc) in enumerate(ACROSS):
            p = slot_of(me, dx, dz, dc)
            out[o] = st_ref[p, :, 0:LANES]
            ends.append(st_ref[p, :, LANES:].astype(jnp.float32))
        rest = st_ref.shape[2] - LANES
        ends.append(jnp.zeros((ends[0].shape[0], LANES - rest * len(ACROSS)), jnp.float32))
        out[len(ACROSS)] = jnp.concatenate(ends, axis=1).astype(out.dtype)


def swap_kernel(many, start, *refs):
    come, go = refs[:many], refs[many:]
    for i, ref in enumerate(come):
        for j, out in enumerate(go):
            out[i] = ref[start + j]


def swap_both_kernel(states, *refs):
    near, packed, outs = refs[: len(NEAR)], refs[len(NEAR) : len(NEAR) + len(FAR)], refs[len(NEAR) + len(FAR) :]
    base = near[0].shape[2]
    rest = states - LANES
    for i, ref in enumerate(near):
        for o, out in enumerate(outs):
            out[i, :, 0:base] = ref[o]
    for d, ref in enumerate(packed):
        ends = ref[len(outs)].astype(jnp.float32)
        for o, out in enumerate(outs):
            out[d, :, base : base + LANES] = ref[o]
            out[d, :, base + LANES : base + states] = ends[:, o * rest : (o + 1) * rest].astype(out.dtype)


def in_vmem(kernel, outs, count, **more):
    return pl.pallas_call(
        kernel,
        out_shape=outs,
        in_specs=[pl.BlockSpec(memory_space=pltpu.VMEM)] * count,
        out_specs=[pl.BlockSpec(memory_space=pltpu.VMEM)] * len(outs),
        compiler_params=pltpu.CompilerParams(vmem_limit_bytes=20 * 2**20),
        **more,
    )


def moved(a, dx, dz, dc):
    pairs = [
        (partner(x, z, c), partner(x + dx, z + dz, c + dc))
        for x in range(SIZE_X)
        for z in range(SIZE_Z)
        for c in range(SIZE_C)
    ]
    return lax.ppermute(a, "mem", pairs)


def gathered(rad, st):
    members, width = rad.shape[1], rad.shape[2]
    wide = width + 2 * LANES
    shape = lambda rows, lanes: [jax.ShapeDtypeStruct((rows, members, lanes), rad.dtype)]
    tall = shape(len(ACROSS), width)
    flat = shape(len(FAR), width)
    sent = shape(len(ACROSS), wide) * (len(NEAR) - 1) + flat * (len(ACROSS) - 1)
    spread = pl.pallas_call(
        spread_kernel,
        out_shape=sent + [pltpu.VMEM(a.shape, a.dtype) for a in shape(len(ACROSS), wide) + flat],
        in_specs=[pl.BlockSpec(memory_space=pltpu.HBM)] * 2,
        out_specs=[pl.BlockSpec(memory_space=pltpu.HBM)] * SENT + [pl.BlockSpec(memory_space=pltpu.VMEM)] * 2,
        scratch_shapes=[pltpu.VMEM(a.shape, a.dtype) for a in sent]
        + [
            pltpu.VMEM(st.shape, st.dtype),
            pltpu.SemaphoreType.DMA((st.shape[0] + 1,)),
            pltpu.SemaphoreType.DMA((SENT,)),
        ],
        compiler_params=pltpu.CompilerParams(vmem_limit_bytes=59 * 10**6),
        name="spread",
    )(rad, st)
    near = spread[: len(NEAR) - 1] + spread[SENT : SENT + 1]
    far = spread[SENT + 1 :] + spread[len(NEAR) - 1 : SENT]
    near = [a if dz == 0 else moved(a, 0, dz, 0) for a, dz in zip(near, NEAR)]
    far = [a if o == (0, 0) else moved(a, o[0], 0, o[1]) for a, o in zip(far, ACROSS)]
    packed = in_vmem(pack_kernel, shape(len(ACROSS) + 1, LANES) * len(FAR), 1)(st)
    packed = [moved(a, 0, dz, 0) for a, dz in zip(packed, FAR)]
    lead = in_vmem(functools.partial(swap_kernel, len(ACROSS), 0), tall, len(ACROSS))(*far)
    lead = [moved(lead[0], 0, FAR[0], 0)]
    rest = tall * (len(FAR) - 1)
    rest = in_vmem(functools.partial(swap_kernel, len(ACROSS), 1), rest, len(ACROSS))(*far)
    far = lead + [moved(a, 0, dz, 0) for a, dz in zip(rest, FAR[1:])]
    both = shape(len(NEAR), wide + 2 * LANES) * len(ACROSS)
    swap_both = in_vmem(functools.partial(swap_both_kernel, st.shape[2]), both, len(NEAR) + len(FAR))
    near = swap_both(*near, *packed)
    near = [a if o == (0, 0) else moved(a, o[0], 0, o[1]) for a, o in zip(near, ACROSS)]
    rows = members * len(ACROSS)
    sums = in_vmem(
        functools.partial(early_kernel, st.shape[2]),
        [
            jax.ShapeDtypeStruct((rows * len(FAR), 2 * LANES), rad.dtype),
            jax.ShapeDtypeStruct((st.shape[2], width), jnp.float32),
        ],
        len(ACROSS),
        scratch_shapes=[pltpu.VMEM((rows * len(NEAR), wide), rad.dtype)],
    )(*near)
    return list(far) + list(sums)


def early_kernel(states, *refs):
    near, (far_ref, cross_ref, x_ref) = refs[:-3], refs[-3:]
    width = cross_ref.shape[1]
    wide = x_ref.shape[1]
    members = near[0].shape[1]
    block = members * len(NEAR)
    for o, part in enumerate(near):
        x_ref[o * block : (o + 1) * block, :] = part[:, :, 0:wide].reshape(block, wide)
        for k in range(len(FAR)):
            row = (k * len(ACROSS) + o) * members
            far_ref[row : row + members, 0:states] = part[k, :, wide : wide + states]
    tn = (((0,), (0,)), ((), ()))
    st = x_ref[:, width : width + states]
    cross_ref[...] = lax.dot_general(st, x_ref[:, 0:width], tn, preferred_element_type=jnp.float32)


def slab_kernel(states, members_all, *refs):
    far, (states_ref, cross_ref, weight_ref, innov_ref, out_ref, x_ref) = refs[:-6], refs[-6:]
    rows = far[0].shape[0] * far[0].shape[1]
    for k, part in enumerate(far):
        x_ref[k * rows : (k + 1) * rows, :] = part[...].reshape(rows, -1)
    tn = (((0,), (0,)), ((), ()))
    st = states_ref[:, 0:states]
    cross = cross_ref[...] + lax.dot_general(st, x_ref[...], tn, preferred_element_type=jnp.float32)
    root = jnp.sqrt(weight_ref[...])
    y = cross * (root * (1.0 / (members_all - 1)))
    y1 = y.astype(jnp.bfloat16)
    y2 = (y - y1.astype(jnp.float32)).astype(jnp.bfloat16)
    nt = (((1,), (1,)), ((), ()))
    main = lax.dot_general(y1, y1, nt, preferred_element_type=jnp.float32)
    side = lax.dot_general(y2, y1, nt, preferred_element_type=jnp.float32)
    info = main + (side + side.T)
    grad = jnp.sum(y * (root * innov_ref[...]), axis=1, keepdims=True)
    r = lax.broadcasted_iota(jnp.int32, info.shape, 0)
    c = lax.broadcasted_iota(jnp.int32, info.shape, 1)
    grad_row = jnp.sum(jnp.where(r == c, grad, 0.0), axis=0, keepdims=True)
    rest = states - LANES
    half = LANES // 2
    other = pltpu.roll(info[half:LANES, 0:LANES], half, 1)
    r, c = places(half)
    out_ref[0:half, :] = jnp.where(c < r, other, info[0:half, 0:LANES])
    out_ref[half:, :] = jnp.zeros((PACKED - half, LANES), jnp.float32)
    out_ref[half : half + rest, :] = info[LANES:states, 0:LANES]
    out_ref[half + rest : half + rest + 1, :] = grad_row[:, 0:LANES]
    out_ref[half + rest + 1 : half + rest + 2, :] = jnp.sum(jnp.where(r == c, other, 0.0), axis=0, keepdims=True)
    out_ref[half + 16 : half + 16 + rest, 0:rest] = info[LANES:states, LANES:states]
    out_ref[half + 16 + rest : half + 17 + rest, 0:rest] = grad_row[:, LANES:states]


def solve_kernel(
    states, a_ref, b_ref, c_ref, d_ref, info_ref, grad_ref, inc_ref, info, grad, inc, left, right, x_ref, r_ref, gj, done
):
    rest = states - LANES
    rows = LANES + 16
    half = LANES // 2
    total = (a_ref[...] + b_ref[...]) + (c_ref[...] + d_ref[...])
    r, c = places(half)
    ra, ca = places(LANES)
    last = jnp.where(ca[0:1] < half, total[half + rest + 1 : half + rest + 2, :], 0.0)
    lower = jnp.where(c < r, total[0:half], 0.0) + jnp.where(c == r, last, 0.0)
    part = jnp.concatenate([jnp.where(c < r, 0.0, total[0:half]), pltpu.roll(lower, half, 1)], axis=0)
    square = jnp.where(ra == ca, part, part + part.T)
    r, c = places(16)
    low = jnp.where(r < rest, total[half : half + 16, :], 0.0)
    corner = jnp.where((r < rest) & (c < rest), total[half + 16 : half + 32, :], 0.0)
    g0 = total[half + rest : half + rest + 1, :]
    g1 = total[half + 16 + rest : half + 17 + rest, :]
    upper = jnp.concatenate([low, jnp.zeros((LANES - 16, LANES), jnp.float32)], axis=0).T
    info[:, 0, 0:LANES] = jnp.concatenate([square, low[0:rest]], axis=0)
    info[:, 0, LANES:states] = jnp.concatenate([upper[:, 0:rest], corner[0:rest, 0:rest]], axis=0)
    grad[:, 0:LANES] = g0
    grad[:, LANES:states] = g1[:, 0:rest]
    eye = (ra == ca).astype(jnp.float32)
    eye_low = (r == c).astype(jnp.float32)
    left[0:LANES, :] = square + eye
    left[LANES:rows, :] = low
    right[0:LANES, :] = upper
    right[LANES:rows, :] = corner + eye_low
    early = (
        pltpu.make_async_copy(info, info_ref, done.at[0]),
        pltpu.make_async_copy(grad, grad_ref, done.at[1]),
    )
    for copy in early:
        copy.start()

    def to_rows(v):
        return (
            jnp.sum(v[0:LANES] * eye, axis=0, keepdims=True),
            jnp.sum(v[LANES:rows] * eye_low, axis=0, keepdims=True),
        )

    def times(v):
        v0, v1 = to_rows(v)
        return jnp.broadcast_to(jnp.sum(left[...] * v0 + right[...] * v1, axis=1, keepdims=True), (rows, LANES))

    def dot(u, v):
        return jnp.sum(u * v, axis=0, keepdims=True)

    def ratio(num, den):
        return jnp.where(den > 0.0, num / jnp.where(den > 0.0, den, 1.0), 0.0)

    def steps(n, x, res, p, s, gamma, alpha):
        for _ in range(n):
            w = times(res)
            new = dot(res, res)
            delta = dot(res, w)
            if gamma is None:
                alpha = ratio(new, delta)
                p, s = res, w
            else:
                beta = ratio(new, gamma)
                alpha = ratio(new, delta - beta * ratio(new, alpha))
                p = res + beta * p
                s = w + beta * s
            x = x + alpha * p
            res = res - alpha * s
            gamma = new
        return x, res

    col = jnp.concatenate(
        [
            jnp.broadcast_to(jnp.sum(eye * g0, axis=1, keepdims=True), (LANES, LANES)),
            jnp.broadcast_to(jnp.sum(jnp.where(c < rest, eye_low * g1, 0.0), axis=1, keepdims=True), (16, LANES)),
        ],
        axis=0,
    )

    def put(x):
        x0, x1 = to_rows(x)
        inc[:, 0:LANES] = x0
        inc[:, LANES:states] = x1[:, 0:rest]

    def open_after(x):
        res = col - times(x)
        bad = jnp.logical_not(dot(res, res) <= (TOL * TOL) * dot(x, x))
        return jnp.max(bad[:, 0:1].astype(jnp.int32)), res

    x, _ = steps(FIRST_STEPS, jnp.zeros_like(col), col, None, None, None, None)
    put(x)
    still, res = open_after(x)

    @pl.when(still > 0)
    def _():
        x_ref[...] = x
        r_ref[...] = res

        def more(state):
            k, _ = state
            x, _ = steps(MORE_STEPS, x_ref[...], r_ref[...], None, None, None, None)
            still, res = open_after(x)
            x_ref[...] = x
            r_ref[...] = res
            return k + 1, still

        _, open_still = lax.while_loop(
            lambda s: (s[0] < MORE_ROUNDS) & (s[1] > 0), more, (jnp.int32(0), jnp.int32(1))
        )
        put(x_ref[...])

        @pl.when(open_still > 0)
        def _():
            wide_r = lax.broadcasted_iota(jnp.int32, (rows, 3 * LANES), 0)
            wide_c = lax.broadcasted_iota(jnp.int32, (rows, 3 * LANES), 1)
            gj[:, 0:LANES] = left[...]
            gj[:, LANES : 2 * LANES] = right[...]
            gj[:, 2 * LANES : 3 * LANES] = col

            def eliminate(i, _):
                a = gj[...]
                row = jnp.sum(jnp.where(wide_r == i, a, 0.0), axis=0, keepdims=True)
                lane = lax.broadcasted_iota(jnp.int32, row.shape, 1)
                pivot = jnp.sum(jnp.where(lane == i, row, 0.0), axis=1, keepdims=True)
                row = row / pivot
                column = jnp.sum(jnp.where(wide_c == i, a, 0.0), axis=1, keepdims=True)
                gj[...] = jnp.where(wide_r == i, row, a - column * row)
                return 0

            lax.fori_loop(0, states, eliminate, 0)
            put(gj[:, 2 * LANES : 3 * LANES])

    late = pltpu.make_async_copy(inc, inc_ref, done.at[2])
    late.start()
    for copy in early:
        copy.wait()
    late.wait()


def shards(state_anom, radiance_anom, inv_noise, innovation, valid_count):
    _, local_members, states = state_anom.shape
    slab_width = radiance_anom.shape[2]
    mem = lax.axis_size("mem")
    chan = lax.axis_size("chan")
    members_all = local_members * mem
    f32 = jnp.float32
    blocks = gathered(radiance_anom, state_anom)
    prof = lax.axis_index("mem")
    own_count = lax.dynamic_slice_in_dim(valid_count, prof, 1, 0)
    slots = lax.axis_index("chan") * slab_width + jnp.arange(slab_width, dtype=jnp.int32)
    weight = jnp.where(slots[None, :] < own_count[:, None], inv_noise[None, :], 0.0)
    innov = lax.dynamic_slice_in_dim(innovation, prof, 1, 0)
    part = pl.pallas_call(
        functools.partial(slab_kernel, states, members_all),
        out_shape=jax.ShapeDtypeStruct((PACKED, LANES), f32),
        in_specs=[pl.BlockSpec(memory_space=pltpu.VMEM)] * (len(blocks) + 2),
        out_specs=pl.BlockSpec(memory_space=pltpu.VMEM),
        scratch_shapes=[pltpu.VMEM(blocks[-2].shape[:1] + (slab_width,), jnp.bfloat16)],
        compiler_params=pltpu.CompilerParams(vmem_limit_bytes=24 * 2**20),
        name="slab",
    )(*blocks, weight, innov)
    parts = [part] + [
        lax.ppermute(part, "chan", [(j, (j + k) % chan) for j in range(chan)]) for k in (2, 1, 3)
    ]
    outs = [(states, 1, states), (1, states), (1, states)]
    square = pltpu.VMEM((LANES + 16, LANES), f32)
    info, grad, inc = pl.pallas_call(
        functools.partial(solve_kernel, states),
        out_shape=[jax.ShapeDtypeStruct(shape, f32) for shape in outs],
        in_specs=[pl.BlockSpec(memory_space=pltpu.VMEM)] * 4,
        out_specs=[pl.BlockSpec(memory_space=pltpu.HBM)] * 3,
        scratch_shapes=[pltpu.VMEM(shape, f32) for shape in outs]
        + [square] * 4
        + [pltpu.VMEM((LANES + 16, 3 * LANES), f32), pltpu.SemaphoreType.DMA((3,))],
        compiler_params=pltpu.CompilerParams(vmem_limit_bytes=8 * 2**20),
        name="solve",
    )(*parts)
    return (jnp.transpose(info, (1, 0, 2)), grad, inc)


def solution(mesh):
    in_specs = (P(None, "mem", None), P(None, "mem", "chan"), P("chan"), P(None, "chan"), P())
    out_specs = (P("mem", None, None), P("mem", None), P("mem", None))
    return jax.shard_map(shards, mesh=mesh, in_specs=in_specs, out_specs=out_specs, check_vma=False)
```
